32 devices in a mesh: band: 8 (over z, y), dom: 4 (over x, core).
Axes of the slice: x: 2, y: 2, z: 4, core: 2. Of those that a mesh axis runs over, the one named last changes fastest.
Arguments:
- wavefunctions: float32 [1024, 16, 16, 128], P('band', 'dom'), may hold values from -6 to 6
- potential: float32 [16, 16, 128], P('dom'), may hold values from -40 to 40
- projectors: float32 [16, 18, 4, 16, 128], P('dom'), may hold values from -0.0625 to 0.0625
- hamiltonian_correction: float32 [16, 18, 18], P('dom'), may hold values from -0.078125 to 0.078125
- delta_s: float32 [16, 18, 18], P('dom'), may hold values from -0.078125 to 0.078125
- projector_count: int32 [16], P('dom'), may hold values from 1 to 18
Outputs:
- ham: float32 [1024, 1024], P('band')
- correlation: float32 [1024, 1024], P('band')
The draws below stay inside these ranges and needn't reach their ends.
All inputs are finite; a program needn't handle non-finite values.
Results may differ from the reference program's by a relative error of at most 0.00007.
Values sent between devices are 32-bit elements; how exact they have to be, the bound alone decides.
A program may use at most 192 MiB of HBM per device.

```python
import jax
import jax.numpy as jnp
from jax import lax

BANDS = 1024
NPROJ = 18
A_DEV = 4
CX = 4
NY = 16
NZ = 128
NX = 16
ATOMS = 16
N_DOM = 4


def place_ends(entries, rng, least, largest):
    extent = entries.shape
    index_at = [jax.random.randint(jax.random.fold_in(rng, axis), (), 0, extent[axis]) for axis in range(len(extent))]
    entries = entries.at[tuple(index_at)].set(least)
    longest = extent.index(max(extent))
    index_at[longest] = (index_at[longest] + 1) % extent[longest]
    return entries.at[tuple(index_at)].set(largest)


def block_levels(rng, dims, pieces, least, top_value):
    gain = 1.0
    for axis_at, parts in pieces:
        heights = jax.random.uniform(jax.random.fold_in(jax.random.fold_in(rng, 6), axis_at), (parts,), jnp.float32, least / len(pieces), top_value / len(pieces))
        gain = gain * jnp.repeat(jnp.exp(heights), dims[axis_at] // parts).reshape((-1,) + (1,) * (len(dims) - 1 - axis_at))
    return gain


def centred(stream_key, shape, deviation, reach, cuts=(), kind=jnp.bfloat16):
    result = deviation * jax.random.normal(stream_key, shape, jnp.float32)
    if cuts:
        result = result * block_levels(stream_key, shape, cuts, -0.22, 0.18)
    return jnp.clip(result, -reach, reach).astype(kind)


def setup_inputs(seed: int = 0) -> dict:
    arg_keys = jax.random.split(jax.random.key(seed), 7)
    return {
        "wavefunctions": centred(arg_keys[0], (BANDS, NX, NY, NZ), 1.0, 6.0, ((0, 8), (1, 4)), jnp.float32),
        "potential": jnp.clip(jax.random.uniform(arg_keys[1], (NX, NY, NZ), jnp.float32, -40.0, 40.0) * block_levels(arg_keys[1], (NX, NY, NZ), ((0, 4),), -0.4, 0.0), -40.0, 40.0),
        "projectors": centred(arg_keys[2], (ATOMS, NPROJ, CX, NY, NZ), (CX * NY * NZ) ** -0.5, 0.0625, ((0, 4),), jnp.float32),
        "hamiltonian_correction": centred(arg_keys[3], (ATOMS, NPROJ, NPROJ), (ATOMS * NPROJ * NPROJ) ** -0.5, 0.078125, ((0, 4),), jnp.float32),
        "delta_s": centred(arg_keys[4], (ATOMS, NPROJ, NPROJ), (ATOMS * NPROJ * NPROJ) ** -0.5, 0.078125, ((0, 4),), jnp.float32),
        "projector_count": place_ends(jax.random.randint(arg_keys[5], (ATOMS,), 1, NPROJ + 1), jax.random.fold_in(arg_keys[5], 1), 1, NPROJ).astype(jnp.int32),
    }


def rows_product(left, right):
    return lax.dot_general(left, right, (((1,), (1,)), ((), ())), precision=lax.Precision.HIGHEST, preferred_element_type=jnp.float32)


def reference(wavefunctions, potential, projectors, hamiltonian_correction, delta_s, projector_count):
    bands = wavefunctions.shape[0]
    beside = jnp.roll(wavefunctions, 1, 1) + jnp.roll(wavefunctions, -1, 1)
    beside = beside + jnp.roll(wavefunctions, 1, 2) + jnp.roll(wavefunctions, -1, 2)
    beside = beside + jnp.roll(wavefunctions, 1, 3) + jnp.roll(wavefunctions, -1, 3)
    hpsi = 0.5 * (6.0 * wavefunctions - beside) + potential[None] * wavefunctions
    volume = 1.0 / (NX * NY * NZ)
    local_cells = CX * NY * NZ
    split_psi = wavefunctions.reshape(bands, N_DOM, local_cells)
    split_proj = projectors.reshape(N_DOM, A_DEV * NPROJ, local_cells)
    projector_coefficient = jnp.einsum("bdg,dkg->bdk", split_psi, split_proj, precision=lax.Precision.HIGHEST)
    slot_mask = (jnp.arange(NPROJ, dtype=jnp.int32)[None, :] < projector_count[:, None]).astype(jnp.float32)
    projector_coefficient = projector_coefficient.reshape(bands, ATOMS, NPROJ) * slot_mask[None]
    sym_h = 0.5 * (hamiltonian_correction + jnp.swapaxes(hamiltonian_correction, 1, 2))
    sym_s = 0.5 * (delta_s + jnp.swapaxes(delta_s, 1, 2))
    coupled_h = jnp.einsum("bap,apq->baq", projector_coefficient, sym_h, precision=lax.Precision.HIGHEST).reshape(bands, -1)
    coupled_s = jnp.einsum("bap,apq->baq", projector_coefficient, sym_s, precision=lax.Precision.HIGHEST).reshape(bands, -1)
    coef_flat = projector_coefficient.reshape(bands, -1)
    psi_flat = wavefunctions.reshape(bands, -1)
    hpsi_flat = hpsi.reshape(bands, -1)
    ham = volume * rows_product(hpsi_flat, psi_flat) + rows_product(coupled_h, coef_flat)
    correlation = volume * rows_product(psi_flat, psi_flat) + rows_product(coupled_s, coef_flat)
    return ham, correlation
```

```python
import functools

import jax
import jax.numpy as jnp
from jax import lax
from jax.experimental import pallas as pl
from jax.experimental.pallas import tpu as pltpu
from jax.sharding import PartitionSpec as P

MESH = pl.DeviceIdType.MESH
CONTRACT_LAST = (((1,), (1,)), ((), ()))
MATMUL = (((1,), (0,)), ((), ()))
QUADS = 4


def parts(value):
    high = value.astype(jnp.bfloat16)
    low = (value - high.astype(jnp.float32)).astype(jnp.bfloat16)
    return high, low


def three(left, right, dims, axis):
    (left_high, left_low), (right_high, right_low) = left, right
    return lax.dot_general(
        jnp.concatenate([left_high, left_high, left_low], axis=1),
        jnp.concatenate([right_high, right_low, right_high], axis=axis),
        dims, preferred_element_type=jnp.float32,
    )


def exact(left, right):
    return lax.dot_general(
        left, right, MATMUL, precision=lax.Precision.HIGHEST, preferred_element_type=jnp.float32
    )


def gram_kernel(lines, doms, fused, volume, counts, psi_in, pot, proj_in, ham_corr, delta, result, *scratch):
    (
        nat, packed, partner, halo, partner_halo, slots_r, slots_l, lhs_high, lhs_low,
        own_edge, left_edge, edges_r, edges_l, proj, sym, coef, coef_below, coup_high, coup_low,
        load_sem, proj_sem, swap_send, swap_recv, halo_send, halo_recv, fwd_send, fwd_recv,
        right_send, right_recv, left_send, left_recv,
        right_edge_send, right_edge_recv, left_edge_send, left_edge_recv,
        coef_send, coef_recv, pair_send, pair_recv,
    ) = scratch[:39]
    rows, bands, nz = nat.shape
    cx, ny = pot.shape[:2]
    lane_half = nz // 2
    half = rows // 2
    per_y = cx // 2
    steps = ny // 2
    phases = lines - 2
    hops = lines - 1
    last = lines - 1
    atoms, slots = ham_corr.shape[:2]
    used = atoms * slots
    live = -(-used // 8) * 8
    width = sym.shape[1]
    grid = scratch[39] if fused else result

    mine = lax.axis_index("band")
    dom = lax.axis_index("dom")
    line = mine // 2
    side = mine % 2
    pair = line * 2 + (1 - side)
    upper = jnp.minimum(line + 1, last) * 2 + side
    lower = jnp.maximum(line - 1, 0) * 2 + side
    dom_next = (dom + 1) % doms
    dom_prev = (dom + doms - 1) % doms

    def loads(y):
        copies = []
        for p in range(cx):
            r = y * cx + p
            copies.append(pltpu.make_async_copy(psi_in.at[:, p, y], nat.at[r], load_sem.at[r]))
        return copies

    def proj_loads(y):
        copies = []
        for p in range(cx):
            r = y * cx + p
            copies.append(pltpu.make_async_copy(proj_in.at[:, p, y], proj.at[r], proj_sem.at[r]))
        return copies

    def start_loads(y, carry):
        for copy in loads(y):
            copy.start()
        return carry

    def start_proj(y, carry):
        for copy in proj_loads(y):
            copy.start()
        return carry

    lax.fori_loop(0, ny, start_loads, 0)
    lax.fori_loop(0, ny, start_proj, 0)

    barrier = pltpu.get_barrier_semaphore()
    pl.semaphore_signal(barrier, inc=1, device_id={"band": pair}, device_id_type=MESH)
    for ahead in range(1, lines):
        there = (line + ahead) % lines * 2 + side
        pl.semaphore_signal(barrier, inc=1, device_id={"band": there}, device_id_type=MESH)
    for ahead in range(1, doms):
        pl.semaphore_signal(barrier, inc=1, device_id={"dom": (dom + ahead) % doms}, device_id_type=MESH)
    pl.semaphore_wait(barrier, 1 + hops + doms - 1)

    def remote(src, dst, send, recv, where):
        return pltpu.make_async_remote_copy(
            src_ref=src, dst_ref=dst, send_sem=send, recv_sem=recv,
            device_id=where, device_id_type=MESH,
        )

    def swap(y):
        at = pl.ds(y * cx, cx)
        return remote(nat.at[at], partner.at[at], swap_send.at[y], swap_recv.at[y], {"band": pair})

    def planes(src, dst, send, recv, y):
        return [
            remote(src.at[y * cx + p], dst.at[edge, y], send.at[edge, y], recv.at[edge, y], {"dom": to})
            for edge, p, to in ((0, cx - 1, dom_next), (1, 0, dom_prev))
        ]

    def halos(y):
        return planes(nat, halo, halo_send, halo_recv, y)

    def forwards(y):
        return planes(partner, partner_halo, fwd_send, fwd_recv, y)

    class Way:
        def __init__(self, base, place, slots, edges, send, recv, edge_send, edge_recv, to):
            self.base, self.place, self.slots, self.edges = base, place, slots, edges
            self.send, self.recv, self.edge_send, self.edge_recv, self.to = send, recv, edge_send, edge_recv, to
            self.count = jnp.where(place == 0, 0, jnp.where(place == 1, 2, jnp.where(place == last, last - 1, place)))
            self.own_first = place < last - 1
            self.shift = jnp.where(self.own_first, 1, 0)

        def source(self, f):
            from_place = jnp.where(
                self.place == 1, 0, jnp.where(self.place == last, self.place - 2 - f, self.place - 1 - f)
            )
            from_place = jnp.clip(from_place, 0, last)
            return from_place if self.base == 0 else last - from_place

        def half_of(self, f):
            return jnp.where(self.place == 1, 1 - self.base, self.base) if f == 1 else self.base

        def gets(self, f):
            return self.count > f

        def gets_edge(self, f):
            return (self.count > f) & (self.place != 1) if f else self.count > 0

        def passes(self, f):
            return (self.place >= 1) & (self.place < last) & (self.place > f)

        def own(self, y):
            at = pl.ds(y * per_y, per_y)
            return remote(
                packed.at[self.base, at], self.slots.at[0, at], self.send.at[0, y], self.recv.at[0, y], {"band": self.to}
            )

        def extra(self, y):
            at = pl.ds(y * per_y, per_y)
            return remote(
                packed.at[1 - self.base, at], self.slots.at[1, at], self.send.at[1, y], self.recv.at[1, y],
                {"band": self.to},
            )

        def hop(self, f, y):
            at = pl.ds(y * per_y, per_y)
            q = jnp.minimum(f + self.shift, phases - 1)
            return remote(
                self.slots.at[f, at], self.slots.at[q, at], self.send.at[q, y], self.recv.at[q, y], {"band": self.to}
            )

        def arrival(self, f, y):
            at = pl.ds(y * per_y, per_y)
            return remote(
                self.slots.at[f, at], self.slots.at[f, at], self.send.at[f, y], self.recv.at[f, y], {"band": self.to}
            )

        def own_edge(self):
            return remote(own_edge, self.edges.at[0], self.edge_send.at[0], self.edge_recv.at[0], {"band": self.to})

        def edge_hop(self, f):
            q = jnp.minimum(f + self.shift, phases - 1)
            return remote(
                self.edges.at[f], self.edges.at[q], self.edge_send.at[q], self.edge_recv.at[q], {"band": self.to}
            )

        def edge_arrival(self, f):
            return remote(
                self.edges.at[f], self.edges.at[f], self.edge_send.at[f], self.edge_recv.at[f], {"band": self.to}
            )

    ways = (
        Way(0, line, slots_r, edges_r, right_send, right_recv, right_edge_send, right_edge_recv, upper),
        Way(1, last - line, slots_l, edges_l, left_send, left_recv, left_edge_send, left_edge_recv, lower),
    )
    live_rows = pl.ds(0, live)
    coef_swap = remote(
        coef.at[0, live_rows], coef.at[1, live_rows], pair_send.at[0], pair_recv.at[0], {"band": pair}
    )

    def coef_hop(dist):
        src = coef.at[0, live_rows] if dist == 1 else coef_below.at[dist - 2, live_rows]
        return remote(
            src, coef_below.at[dist - 1, live_rows], coef_send.at[dist - 1], coef_recv.at[dist - 1], {"band": upper}
        )

    lanes = lax.broadcasted_iota(jnp.int32, (bands, nz), 1)
    low_lanes = lanes < lane_half

    def pack(first, second):
        return (
            jnp.where(low_lanes, first, pltpu.roll(second, lane_half, 1)),
            jnp.where(low_lanes, pltpu.roll(first, lane_half, 1), second),
        )

    def start_own(y):
        for way in ways:
            @pl.when(way.own_first)
            def _(way=way):
                way.own(y).start()

    own_edge[...] = jnp.zeros_like(own_edge)
    left_edge[...] = jnp.zeros_like(left_edge)

    def begin(y, carry):
        for copy in loads(y):
            copy.wait()
        swap(y).start()
        for copy in halos(y):
            copy.start()
        for pp in range(per_y):
            k = y * per_y + pp
            first, second = pack(nat[2 * k], nat[2 * k + 1])
            packed[0, k] = first
            packed[1, k] = second

        @pl.when((y >= 1) & (y <= steps))
        def _():
            start_own(y - 1)

        return carry

    lax.fori_loop(0, ny, begin, 0)

    def gather_edge(r, carry):
        here = nat[r]
        spot = (lanes == r) | (lanes == r + lane_half)
        return jnp.where(spot, pltpu.roll(here, (r + lane_half) % nz, 1), carry)

    own_edge[...] = lax.fori_loop(0, rows, gather_edge, jnp.zeros((bands, nz), jnp.float32))

    for kind, source in enumerate((ham_corr, delta)):
        total = jnp.zeros((width, width), jnp.float32)
        for a in range(atoms):
            wide = lax.broadcasted_iota(jnp.int32, (slots, width), 0) + a * slots
            place = wide == lax.broadcasted_iota(jnp.int32, (slots, width), 1)
            place = place & (wide - a * slots < counts[a])
            tall = lax.broadcasted_iota(jnp.int32, (width, slots), 1) + a * slots
            tall_place = tall == lax.broadcasted_iota(jnp.int32, (width, slots), 0)
            tall_place = tall_place & (tall - a * slots < counts[a])
            total = total + exact(tall_place.astype(jnp.float32), exact(source[a], place.astype(jnp.float32)))
        sym[kind] = (0.5 / volume) * (total + jnp.transpose(total))

    coef[0] = jnp.zeros((width, bands), jnp.float32)
    if live < width:
        unused = jnp.zeros((width - live, bands), jnp.float32)
        coef[1, pl.ds(live, width - live)] = unused
        for slot in range(hops):
            coef_below[slot, pl.ds(live, width - live)] = unused

    def coef_body(y, carry):
        for copy in proj_loads(y):
            copy.wait()
        left, right = [], []
        for p in range(cx):
            r = y * cx + p
            proj_high, proj_low = parts(proj[r])
            high, low = parts(nat[r])
            left += [proj_high, proj_high, proj_low]
            right += [high, low, high]
        coef[0, pl.ds(0, used)] += lax.dot_general(
            jnp.concatenate(left, axis=1), jnp.concatenate(right, axis=1), CONTRACT_LAST,
            preferred_element_type=jnp.float32,
        )
        return carry

    lax.fori_loop(0, ny, coef_body, 0)

    for way in ways:
        @pl.when(way.own_first)
        def _(way=way):
            way.own_edge().start()

    coef_swap.start()

    @pl.when(line < last)
    def _():
        coef_hop(1).start()

    def start_rest(y, carry):
        start_own(y)
        return carry

    lax.fori_loop(steps, ny, start_rest, 0)
    for way in ways:
        @pl.when(way.place == 0)
        def _(way=way):
            def body(y, carry):
                way.extra(y).start()
                return carry

            lax.fori_loop(0, ny, body, 0)

    grid[...] = jnp.zeros_like(grid)

    def operand(src, edges, group, y):
        up = (y + ny - 1) % ny
        down = (y + 1) % ny
        edge = left_edge[group]
        for pp in range(per_y):
            k = y * per_y + pp
            hpsi, own = [], []
            for t in range(2):
                p = 2 * pp + t
                r = y * cx + p
                here = src[r]
                before = edges[0, y] if p == 0 else src[r - 1]
                after = edges[1, y] if p == cx - 1 else src[r + 1]
                beside = before + after
                beside = beside + src[up * cx + p]
                beside = beside + src[down * cx + p]
                beside = beside + jnp.where(lanes % lane_half == 0, 0.0, pltpu.roll(here, 1, 1))
                beside = beside + pltpu.roll(here, nz - 1, 1)
                hpsi.append(0.5 * (6.0 * here - beside) + pot[p, pl.ds(y, 1)] * here)
                own.append(here)
                spot = (lanes == r) | (lanes == r + lane_half)
                edge = jnp.where(spot, -0.5 * pltpu.roll(here, (r + lane_half + 1) % nz, 1), edge)
            for slot, both in ((2 * group, pack(*hpsi)), (2 * group + 1, pack(*own))):
                for h in range(2):
                    high, low = parts(both[h])
                    lhs_high[h * half + k, pl.ds(slot * bands, bands)] = high
                    lhs_low[h * half + k, pl.ds(slot * bands, bands)] = low
        left_edge[group] = edge

    def accumulate(group, source, row, right_row, count):
        where = pl.ds(group * 2 * bands, 2 * bands)
        left, right = [], []
        for i in range(count):
            high, low = lhs_high[row + i, where], lhs_low[row + i, where]
            other_high, other_low = right_row(i)
            left += [high, high, low]
            right += [other_high, other_low, other_high]
        grid[source, where] += lax.dot_general(
            jnp.concatenate(left, axis=1), jnp.concatenate(right, axis=1), CONTRACT_LAST,
            preferred_element_type=jnp.float32,
        )

    def with_own(group, y, ys):
        own = pl.ds(bands, bands)
        for h in range(2):
            row = h * half + y * per_y
            accumulate(
                group, line, row, lambda i, row=row: (lhs_high[row + i, own], lhs_low[row + i, own]), ys * per_y
            )

    def with_moved(group, way, f, y, ys):
        accumulate(
            group, way.source(f), way.half_of(f) * half + y * per_y,
            lambda i: parts(way.slots[f, y * per_y + i]), ys * per_y,
        )

    def moved_all(group, f, y, ys):
        for way in ways:
            @pl.when(way.gets(f))
            def _(way=way):
                with_moved(group, way, f, y, ys)

    def take(f, t):
        for y in (2 * t, 2 * t + 1):
            for way in ways:
                @pl.when(way.gets(f))
                def _(way=way, y=y):
                    way.arrival(f, y).wait_recv()

                @pl.when(way.passes(f))
                def _(way=way, y=y):
                    way.hop(f, y).start()

    def partner_operand(y):
        for copy in forwards(y):
            copy.wait_recv()
        operand(partner, partner_halo, 1, y)

    def with_edges(group):
        into = pl.ds(2 * group * bands, bands)
        left = parts(left_edge[group])
        grid[line, into] += three(left, parts(own_edge[...]), CONTRACT_LAST, 1)
        for way in ways:
            for f in range(phases):
                @pl.when(way.gets_edge(f))
                def _(way=way, f=f):
                    keep = (low_lanes if way.base == 0 else ~low_lanes) | (way.place == 1)
                    grid[way.source(f), into] += three(
                        left, parts(jnp.where(keep, way.edges[f], 0.0)), CONTRACT_LAST, 1
                    )

    def edge_stage(f):
        for way in ways:
            @pl.when(way.gets_edge(f))
            def _(way=way):
                way.edge_arrival(f).wait_recv()

            @pl.when(way.passes(f))
            def _(way=way):
                way.edge_hop(f).start()

    def couple(group):
        for kind in range(2):
            coupled = jnp.transpose(exact(sym[kind], coef[group]))
            high, low = parts(coupled)
            where = pl.ds((2 * group + kind) * bands, bands)
            coup_high[where] = high
            coup_low[where] = low

    def project(source, right):
        grid[source] += three((coup_high[...], coup_low[...]), parts(right), MATMUL, 0)

    def coef_stage(dist):
        @pl.when(line >= dist)
        def _():
            coef_hop(dist).wait_recv()

        if dist < hops:
            @pl.when((line >= dist) & (line < last))
            def _():
                coef_hop(dist + 1).start()

        @pl.when(line >= dist)
        def _():
            project(line - dist, coef_below[dist - 1])

    def partner_row(u):
        swap(u).wait_recv()
        for copy in forwards(u):
            copy.start()

        @pl.when(u >= 2)
        def _():
            partner_operand(u - 1)
            with_own(1, u - 1, 1)
            moved_all(1, 0, u - 1, 1)

    def first_phase(t, carry):
        for y in (2 * t, 2 * t + 1):
            for copy in halos(y):
                copy.wait_recv()
            operand(nat, halo, 0, y)
        with_own(0, 2 * t, 2)
        take(0, t)
        moved_all(0, 0, 2 * t, 2)
        partner_row(t)
        return carry

    lax.fori_loop(0, steps, first_phase, 0)

    coef_swap.wait_recv()
    couple(0)
    couple(1)
    project(line, coef[0])
    edge_stage(0)
    coef_stage(1)

    def second_phase(t, carry):
        take(1, t)
        moved_all(0, 1, 2 * t, 2)
        partner_row(steps + t)
        for y in (2 * t, 2 * t + 1):
            @pl.when((y != 0) & (y != ny - 1))
            def _(y=y):
                moved_all(1, 1, y, 1)

        for stage in range(1, hops):
            @pl.when(t == min(2 * stage, steps - 2))
            def _(stage=stage):
                if stage < phases:
                    edge_stage(stage)
                coef_stage(stage + 1)

        @pl.when(t == steps - 2)
        def _():
            with_edges(0)

        return carry

    lax.fori_loop(0, steps, second_phase, 0)
    for y in (0, ny - 1):
        partner_operand(y)
        with_own(1, y, 1)
        moved_all(1, 0, y, 1)
        moved_all(1, 1, y, 1)
    with_edges(1)
    for f in range(2, phases):
        def later_phase(t, carry, f=f):
            take(f, t)
            moved_all(0, f, 2 * t, 2)
            moved_all(1, f, 2 * t, 2)
            return carry

        lax.fori_loop(0, steps, later_phase, 0)

    if fused:
        combine(
            lines, volume, grid, result, remote, line, side, pair, dom, scratch[40:],
        )

    def finish(y, carry):
        swap(y).wait_send()
        for copy in halos(y) + forwards(y):
            copy.wait_send()
        for way in ways:
            @pl.when(way.own_first)
            def _(way=way):
                way.own(y).wait_send()

            @pl.when(way.place == 0)
            def _(way=way):
                way.extra(y).wait_send()

            for f in range(phases):
                @pl.when(way.passes(f))
                def _(way=way, f=f):
                    way.hop(f, y).wait_send()

        return carry

    lax.fori_loop(0, ny, finish, 0)
    coef_swap.wait_send()
    for dist in range(1, lines):
        @pl.when((line >= dist - 1) & (line < last))
        def _(dist=dist):
            coef_hop(dist).wait_send()
    for way in ways:
        @pl.when(way.own_first)
        def _(way=way):
            way.own_edge().wait_send()

        for f in range(phases):
            @pl.when(way.passes(f))
            def _(way=way, f=f):
                way.edge_hop(f).wait_send()


def combine(lines, volume, grid, result, remote, line, side, pair, dom, scratch):
    (
        from_core, both, from_chip, total, mirror, swapped,
        core_send, core_recv, chip_send, chip_recv, line_send, line_recv, side_send, side_recv,
        near_send, near_recv, far_send, far_recv, pass_send, pass_recv,
    ) = scratch
    bands = grid.shape[2]
    core = dom % 2
    kind = dom // 2
    other_core = kind * 2 + (1 - core)
    other_chip = (1 - kind) * 2 + core
    mine = pl.ds(pl.multiple_of(core * 2 * bands, bands), 2 * bands)
    theirs = pl.ds(pl.multiple_of((1 - core) * 2 * bands, bands), 2 * bands)
    my_kind = pl.ds(pl.multiple_of(kind * bands, bands), bands)
    their_kind = pl.ds(pl.multiple_of((1 - kind) * bands, bands), bands)

    def to_core(s):
        return remote(grid.at[s, theirs], from_core.at[s], core_send.at[s], core_recv.at[s], {"dom": other_core})

    def to_chip(s):
        return remote(both.at[s, their_kind], from_chip.at[s], chip_send.at[s], chip_recv.at[s], {"dom": other_chip})

    def to_line(s):
        return remote(
            total.at[s], mirror.at[line], line_send.at[s], line_recv.at[line], {"band": s * 2 + side}
        )

    def from_line(s):
        return remote(
            total.at[s], mirror.at[s], line_send.at[s], line_recv.at[s], {"band": s * 2 + side}
        )

    def to_side(s):
        return remote(total.at[s], swapped.at[s], side_send.at[s], side_recv.at[s], {"band": pair})

    def column(s):
        block = s * 2 + jnp.where(core == 0, side, 1 - side)
        return pl.ds(pl.multiple_of(block * bands, bands), bands)

    def piece(s, k, send, recv, to):
        at = result.at[k, :, column(s)]
        return remote(at, at, send.at[s], recv.at[s], {"dom": to})

    def near(s):
        return piece(s, kind, near_send, near_recv, other_core)

    def near_arrival(s):
        block = s * 2 + jnp.where(core == 1, side, 1 - side)
        at = result.at[kind, :, pl.ds(pl.multiple_of(block * bands, bands), bands)]
        return remote(at, at, near_send.at[s], near_recv.at[s], {"dom": other_core})

    def far(s):
        return piece(s, kind, far_send, far_recv, other_chip)

    def far_arrival(s):
        return piece(s, 1 - kind, far_send, far_recv, other_chip)

    def onward(s):
        return piece(s, 1 - kind, pass_send, pass_recv, other_core)

    def onward_arrival(s):
        block = s * 2 + jnp.where(core == 1, side, 1 - side)
        at = result.at[1 - kind, :, pl.ds(pl.multiple_of(block * bands, bands), bands)]
        return remote(at, at, pass_send.at[s], pass_recv.at[s], {"dom": other_core})

    everyone = range(lines)
    for s in everyone:
        to_core(s).start()
    for s in everyone:
        to_core(s).wait_recv()
        both[s] = grid[s, mine] + from_core[s]
        to_chip(s).start()
    for s in everyone:
        to_chip(s).wait_recv()
        total[s] = both[s, my_kind] + from_chip[s]

        @pl.when(line != s)
        def _(s=s):
            to_line(s).start()

        @pl.when(core == 1)
        def _(s=s):
            to_side(s).start()
    for s in everyone:
        @pl.when(core == 1)
        def _(s=s):
            to_side(s).wait_recv()
            result[kind, :, column(s)] = volume * swapped[s]

        @pl.when(core == 0)
        def _(s=s):
            result[kind, :, column(s)] = volume * total[s]

        @pl.when(line != s)
        def _(s=s):
            from_line(s).wait_recv()
            result[kind, :, column(s)] += volume * jnp.transpose(mirror[s])

        near(s).start()
        far(s).start()
    for s in everyone:
        far_arrival(s).wait_recv()
        onward(s).start()
    for s in everyone:
        near_arrival(s).wait_recv()
        onward_arrival(s).wait_recv()
    for s in everyone:
        to_core(s).wait_send()
        to_chip(s).wait_send()
        near(s).wait_send()
        far(s).wait_send()
        onward(s).wait_send()

        @pl.when(line != s)
        def _(s=s):
            to_line(s).wait_send()

        @pl.when(core == 1)
        def _(s=s):
            to_side(s).wait_send()


def gram(psi, pot, proj, ham_corr, delta, counts, lines, doms, fused, volume):
    bands, cx, ny, nz = psi.shape
    rows = cx * ny
    half = rows // 2
    used = proj.shape[0]
    width = -(-used // 128) * 128
    hops = lines - 1
    phases = lines - 2
    f32 = jnp.float32
    dma = pltpu.SemaphoreType.DMA
    vmem = pl.BlockSpec(memory_space=pltpu.VMEM)
    hbm = pl.BlockSpec(memory_space=pl.ANY)
    scratch = [
        pltpu.VMEM((rows, bands, nz), f32),
        pltpu.VMEM((2, half, bands, nz), f32),
        pltpu.VMEM((rows, bands, nz), f32),
        pltpu.VMEM((2, ny, bands, nz), f32),
        pltpu.VMEM((2, ny, bands, nz), f32),
        pltpu.VMEM((phases, half, bands, nz), f32),
        pltpu.VMEM((phases, half, bands, nz), f32),
        pltpu.VMEM((rows, QUADS * bands, nz), jnp.bfloat16),
        pltpu.VMEM((rows, QUADS * bands, nz), jnp.bfloat16),
        pltpu.VMEM((bands, nz), f32),
        pltpu.VMEM((2, bands, nz), f32),
        pltpu.VMEM((phases, bands, nz), f32),
        pltpu.VMEM((phases, bands, nz), f32),
        pltpu.VMEM((rows, used, nz), f32),
        pltpu.VMEM((2, width, width), f32),
        pltpu.VMEM((2, width, bands), f32),
        pltpu.VMEM((hops, width, bands), f32),
        pltpu.VMEM((QUADS * bands, width), jnp.bfloat16),
        pltpu.VMEM((QUADS * bands, width), jnp.bfloat16),
        dma((rows,)), dma((rows,)), dma((ny,)), dma((ny,)), dma((2, ny)), dma((2, ny)), dma((2, ny)), dma((2, ny)),
        dma((phases, ny)), dma((phases, ny)), dma((phases, ny)), dma((phases, ny)),
        dma((phases,)), dma((phases,)), dma((phases,)), dma((phases,)),
        dma((hops,)), dma((hops,)), dma((1,)), dma((1,)),
    ]
    if fused:
        shape = (2, bands, 2 * lines * bands)
        scratch += [
            pltpu.VMEM((lines, QUADS * bands, bands), f32),
            pltpu.VMEM((lines, 2 * bands, bands), f32),
            pltpu.VMEM((lines, 2 * bands, bands), f32),
            pltpu.VMEM((lines, bands, bands), f32),
            pltpu.VMEM((lines, bands, bands), f32),
            pltpu.VMEM((lines, bands, bands), f32),
            pltpu.VMEM((lines, bands, bands), f32),
        ] + [dma((lines,))] * 14
    else:
        shape = (lines, QUADS * bands, bands)
    return pl.pallas_call(
        functools.partial(gram_kernel, lines, doms, fused, volume),
        out_shape=jax.ShapeDtypeStruct(shape, f32),
        in_specs=[pl.BlockSpec(memory_space=pltpu.SMEM), hbm, vmem, hbm, vmem, vmem],
        out_specs=vmem,
        scratch_shapes=scratch,
        compiler_params=pltpu.CompilerParams(
            collective_id=0, has_side_effects=True, vmem_limit_bytes=62 * 1024 * 1024
        ),
    )(counts, psi, pot, proj, ham_corr, delta)


def on_device(
    wavefunctions, potential, projectors, hamiltonian_correction, delta_s, projector_count
):
    bands, cx, ny, nz = wavefunctions.shape
    groups = lax.axis_size("band")
    doms = lax.axis_size("dom")
    lines = groups // 2
    mine = lax.axis_index("band")
    line, side = mine // 2, mine % 2
    volume = 1.0 / (cx * ny * nz * doms)
    atoms, slots = hamiltonian_correction.shape[:2]
    proj = projectors.reshape(atoms * slots, cx, ny, nz)
    fused = doms == QUADS and bands % 128 == 0
    grid = gram(
        wavefunctions, potential, proj, hamiltonian_correction, delta_s, projector_count,
        lines, doms, fused, volume,
    )
    if fused:
        return grid[0], grid[1]
    here = (jnp.arange(lines, dtype=jnp.int32) == line)[:, None, None, None]
    both = lax.psum(grid.reshape(lines, QUADS, bands, bands), "dom")
    lanes = [[at * 2 + s for at in range(lines)] for s in range(2)]
    mirrored = lax.all_to_all(both, "band", 0, 0, axis_index_groups=lanes, tiled=True)
    swapped = lax.ppermute(both, "band", [(i, i ^ 1) for i in range(groups)])
    crossed = (jnp.arange(QUADS, dtype=jnp.int32) >= 2)[None, :, None, None]
    total = volume * jnp.where(crossed, swapped, both) + volume * jnp.where(here, 0.0, jnp.swapaxes(mirrored, 2, 3))
    total = total.reshape(lines, 2, 2, bands, bands)
    by_side = jnp.where(side == 0, total, total[:, ::-1])
    final = jnp.transpose(by_side, (2, 3, 0, 1, 4)).reshape(2, bands, groups * bands)
    return final[0], final[1]


def solution(mesh):
    placed = (
        P("band", "dom", None, None),
        P("dom", None, None),
        P("dom", None, None, None, None),
        P("dom", None, None),
        P("dom", None, None),
        P("dom"),
    )
    return jax.shard_map(
        on_device,
        mesh=mesh,
        in_specs=placed,
        out_specs=(P("band", None), P("band", None)),
        check_vma=False,
    )
```

```python
import functools

import jax
import jax.numpy as jnp
from jax import lax
from jax.experimental import pallas as pl
from jax.experimental.pallas import tpu as pltpu
from jax.sharding import PartitionSpec as P

MESH = pl.DeviceIdType.MESH
CONTRACT_LAST = (((1,), (1,)), ((), ()))
MATMUL = (((1,), (0,)), ((), ()))
QUADS = 4
WINDOW = 8
SWAP_WINDOW = 4
HALO_AHEAD = 6


def parts(value):
    high = value.astype(jnp.bfloat16)
    low = (value - high.astype(jnp.float32)).astype(jnp.bfloat16)
    return high, low


def three(left, right, dims, axis):
    (left_high, left_low), (right_high, right_low) = left, right
    return lax.dot_general(
        jnp.concatenate([left_high, left_high, left_low], axis=1),
        jnp.concatenate([right_high, right_low, right_high], axis=axis),
        dims, preferred_element_type=jnp.float32,
    )


def exact(left, right):
    return lax.dot_general(
        left, right, MATMUL, precision=lax.Precision.HIGHEST, preferred_element_type=jnp.float32
    )


def gram_kernel(lines, doms, fused, volume, counts, psi_in, pot, proj_in, ham_corr, delta, result, *scratch):
    (
        nat, packed, partner, halo, partner_halo, slots_r, slots_l, lhs_high, lhs_low,
        own_edge, left_edge, edges_r, edges_l, proj, sym, coef, coef_below, coup_high, coup_low,
        load_sem, proj_sem, swap_send, swap_recv, halo_send, halo_recv, fwd_send, fwd_recv,
        right_send, right_recv, left_send, left_recv,
        right_edge_send, right_edge_recv, left_edge_send, left_edge_recv,
        coef_send, coef_recv, pair_send, pair_recv,
    ) = scratch[:39]
    rows, bands, nz = nat.shape
    cx, ny = pot.shape[:2]
    lane_half = nz // 2
    half = rows // 2
    per_y = cx // 2
    steps = ny // 2
    phases = lines - 2
    hops = lines - 1
    last = lines - 1
    window = min(WINDOW, ny)
    swap_window = min(SWAP_WINDOW, ny)
    halo_ahead = min(HALO_AHEAD, ny)
    atoms, slots = ham_corr.shape[:2]
    used = atoms * slots
    live = -(-used // 8) * 8
    width = sym.shape[1]
    grid = scratch[39] if fused else result

    mine = lax.axis_index("band")
    dom = lax.axis_index("dom")
    line = mine // 2
    side = mine % 2
    pair = line * 2 + (1 - side)
    upper = jnp.minimum(line + 1, last) * 2 + side
    lower = jnp.maximum(line - 1, 0) * 2 + side
    dom_next = (dom + 1) % doms
    dom_prev = (dom + doms - 1) % doms

    def loads(y):
        copies = []
        for p in range(cx):
            r = y * cx + p
            copies.append(pltpu.make_async_copy(psi_in.at[:, p, y], nat.at[r], load_sem.at[r]))
        return copies

    def proj_loads(y):
        copies = []
        for p in range(cx):
            r = y * cx + p
            copies.append(pltpu.make_async_copy(proj_in.at[:, p, y], proj.at[r], proj_sem.at[r]))
        return copies

    def start_loads(y, carry):
        for copy in loads(y):
            copy.start()
        return carry

    def start_proj(y, carry):
        for copy in proj_loads(y):
            copy.start()
        return carry

    lax.fori_loop(0, ny, start_loads, 0)
    lax.fori_loop(0, ny, start_proj, 0)

    barrier = pltpu.get_barrier_semaphore()
    pl.semaphore_signal(barrier, inc=1, device_id={"band": pair}, device_id_type=MESH)
    for ahead in range(1, lines):
        there = (line + ahead) % lines * 2 + side
        pl.semaphore_signal(barrier, inc=1, device_id={"band": there}, device_id_type=MESH)
    for ahead in range(1, doms):
        pl.semaphore_signal(barrier, inc=1, device_id={"dom": (dom + ahead) % doms}, device_id_type=MESH)
    pl.semaphore_wait(barrier, 1 + hops + doms - 1)

    def remote(src, dst, send, recv, where):
        return pltpu.make_async_remote_copy(
            src_ref=src, dst_ref=dst, send_sem=send, recv_sem=recv,
            device_id=where, device_id_type=MESH,
        )

    def swap(y):
        at = pl.ds(y * cx, cx)
        return remote(nat.at[at], partner.at[at], swap_send.at[y], swap_recv.at[y], {"band": pair})

    def planes(src, dst, send, recv, y):
        return [
            remote(src.at[y * cx + p], dst.at[edge, y], send.at[edge, y], recv.at[edge, y], {"dom": to})
            for edge, p, to in ((0, cx - 1, dom_next), (1, 0, dom_prev))
        ]

    def halos(y):
        return planes(nat, halo, halo_send, halo_recv, y)

    def forwards(y):
        return planes(partner, partner_halo, fwd_send, fwd_recv, y)

    class Way:
        def __init__(self, base, place, slots, edges, send, recv, edge_send, edge_recv, to):
            self.base, self.place, self.slots, self.edges = base, place, slots, edges
            self.send, self.recv, self.edge_send, self.edge_recv, self.to = send, recv, edge_send, edge_recv, to
            self.count = jnp.where(place == 0, 0, jnp.where(place == 1, 2, jnp.where(place == last, last - 1, place)))
            self.own_first = place < last - 1
            self.shift = jnp.where(self.own_first, 1, 0)
            self.items = jnp.where(place == 0, 2, place + 1) * ny

        def source(self, f):
            from_place = jnp.where(
                self.place == 1, 0, jnp.where(self.place == last, self.place - 2 - f, self.place - 1 - f)
            )
            from_place = jnp.clip(from_place, 0, last)
            return from_place if self.base == 0 else last - from_place

        def half_of(self, f):
            return jnp.where(self.place == 1, 1 - self.base, self.base) if f == 1 else self.base

        def gets(self, f):
            return self.count > f

        def gets_edge(self, f):
            return (self.count > f) & (self.place != 1) if f else self.count > 0

        def passes(self, f):
            return (self.place >= 1) & (self.place < last) & (self.place > f)

        def own(self, y):
            at = pl.ds(y * per_y, per_y)
            return remote(
                packed.at[self.base, at], self.slots.at[0, at], self.send.at[0, y], self.recv.at[0, y], {"band": self.to}
            )

        def extra(self, y):
            at = pl.ds(y * per_y, per_y)
            return remote(
                packed.at[1 - self.base, at], self.slots.at[1, at], self.send.at[1, y], self.recv.at[1, y],
                {"band": self.to},
            )

        def hop(self, f, y):
            at = pl.ds(y * per_y, per_y)
            q = jnp.minimum(f + self.shift, phases - 1)
            return remote(
                self.slots.at[f, at], self.slots.at[q, at], self.send.at[q, y], self.recv.at[q, y], {"band": self.to}
            )

        def arrival(self, f, y):
            at = pl.ds(y * per_y, per_y)
            return remote(
                self.slots.at[f, at], self.slots.at[f, at], self.send.at[f, y], self.recv.at[f, y], {"band": self.to}
            )

        def start_item(self, item):
            q, y = item // ny, item % ny

            @pl.when(q == 0)
            def _():
                self.own(y).start()

            @pl.when((q == 1) & (self.place == 0))
            def _():
                self.extra(y).start()

            @pl.when((q >= 1) & (self.place >= 1))
            def _():
                self.hop(jnp.clip(q - 1, 0, phases - 1), y).start()

        def sent(self, item):
            q, y = item // ny, item % ny
            at = pl.ds(y * per_y, per_y)
            remote(
                packed.at[self.base, at], self.slots.at[q, at], self.send.at[q, y], self.recv.at[q, y],
                {"band": self.to},
            ).wait_send()

        def pace(self, u):
            for item in (2 * u + window, 2 * u + window + 1):
                @pl.when(self.own_first & (item < self.items))
                def _(item=item):
                    self.sent(item - window)
                    self.start_item(item)

        def own_edge(self):
            return remote(own_edge, self.edges.at[0], self.edge_send.at[0], self.edge_recv.at[0], {"band": self.to})

        def edge_hop(self, f):
            q = jnp.minimum(f + self.shift, phases - 1)
            return remote(
                self.edges.at[f], self.edges.at[q], self.edge_send.at[q], self.edge_recv.at[q], {"band": self.to}
            )

        def edge_arrival(self, f):
            return remote(
                self.edges.at[f], self.edges.at[f], self.edge_send.at[f], self.edge_recv.at[f], {"band": self.to}
            )

    ways = (
        Way(0, line, slots_r, edges_r, right_send, right_recv, right_edge_send, right_edge_recv, upper),
        Way(1, last - line, slots_l, edges_l, left_send, left_recv, left_edge_send, left_edge_recv, lower),
    )
    live_rows = pl.ds(0, live)
    coef_swap = remote(
        coef.at[0, live_rows], coef.at[1, live_rows], pair_send.at[0], pair_recv.at[0], {"band": pair}
    )

    def coef_hop(dist):
        src = coef.at[0, live_rows] if dist == 1 else coef_below.at[dist - 2, live_rows]
        return remote(
            src, coef_below.at[dist - 1, live_rows], coef_send.at[dist - 1], coef_recv.at[dist - 1], {"band": upper}
        )

    lanes = lax.broadcasted_iota(jnp.int32, (bands, nz), 1)
    low_lanes = lanes < lane_half

    def pack(first, second):
        return (
            jnp.where(low_lanes, first, pltpu.roll(second, lane_half, 1)),
            jnp.where(low_lanes, pltpu.roll(first, lane_half, 1), second),
        )

    def start_own(y):
        for way in ways:
            @pl.when(way.own_first)
            def _(way=way):
                way.own(y).start()

    own_edge[...] = jnp.zeros_like(own_edge)
    left_edge[...] = jnp.zeros_like(left_edge)

    def begin(y, carry):
        for copy in loads(y):
            copy.wait()

        @pl.when(y < swap_window)
        def _():
            swap(y).start()

        @pl.when(y < halo_ahead)
        def _():
            for copy in halos(y):
                copy.start()

        for pp in range(per_y):
            k = y * per_y + pp
            first, second = pack(nat[2 * k], nat[2 * k + 1])
            packed[0, k] = first
            packed[1, k] = second

        @pl.when((y >= 1) & (y <= window))
        def _():
            start_own(y - 1)

        return carry

    lax.fori_loop(0, ny, begin, 0)
    if window == ny:
        start_own(ny - 1)

    def gather_edge(r, carry):
        here = nat[r]
        spot = (lanes == r) | (lanes == r + lane_half)
        return jnp.where(spot, pltpu.roll(here, (r + lane_half) % nz, 1), carry)

    own_edge[...] = lax.fori_loop(0, rows, gather_edge, jnp.zeros((bands, nz), jnp.float32), unroll=8)

    for kind, source in enumerate((ham_corr, delta)):
        total = jnp.zeros((width, width), jnp.float32)
        for a in range(atoms):
            wide = lax.broadcasted_iota(jnp.int32, (slots, width), 0) + a * slots
            place = wide == lax.broadcasted_iota(jnp.int32, (slots, width), 1)
            place = place & (wide - a * slots < counts[a])
            tall = lax.broadcasted_iota(jnp.int32, (width, slots), 1) + a * slots
            tall_place = tall == lax.broadcasted_iota(jnp.int32, (width, slots), 0)
            tall_place = tall_place & (tall - a * slots < counts[a])
            total = total + exact(tall_place.astype(jnp.float32), exact(source[a], place.astype(jnp.float32)))
        sym[kind] = (0.5 / volume) * (total + jnp.transpose(total))

    coef[0] = jnp.zeros((width, bands), jnp.float32)
    if live < width:
        unused = jnp.zeros((width - live, bands), jnp.float32)
        coef[1, pl.ds(live, width - live)] = unused
        for slot in range(hops):
            coef_below[slot, pl.ds(live, width - live)] = unused

    def coef_body(y, carry):
        for copy in proj_loads(y):
            copy.wait()
        left, right = [], []
        for p in range(cx):
            r = y * cx + p
            proj_high, proj_low = parts(proj[r])
            high, low = parts(nat[r])
            left += [proj_high, proj_high, proj_low]
            right += [high, low, high]
        coef[0, pl.ds(0, used)] += lax.dot_general(
            jnp.concatenate(left, axis=1), jnp.concatenate(right, axis=1), CONTRACT_LAST,
            preferred_element_type=jnp.float32,
        )
        return carry

    lax.fori_loop(0, ny, coef_body, 0)

    for way in ways:
        @pl.when(way.own_first)
        def _(way=way):
            way.own_edge().start()

    coef_swap.start()

    @pl.when(line < last)
    def _():
        coef_hop(1).start()

    grid[...] = jnp.zeros_like(grid)

    def operand(src, edges, group, y):
        up = (y + ny - 1) % ny
        down = (y + 1) % ny
        edge = left_edge[group]
        for pp in range(per_y):
            k = y * per_y + pp
            hpsi, own = [], []
            for t in range(2):
                p = 2 * pp + t
                r = y * cx + p
                here = src[r]
                before = edges[0, y] if p == 0 else src[r - 1]
                after = edges[1, y] if p == cx - 1 else src[r + 1]
                beside = before + after
                beside = beside + src[up * cx + p]
                beside = beside + src[down * cx + p]
                beside = beside + jnp.where(lanes % lane_half == 0, 0.0, pltpu.roll(here, 1, 1))
                beside = beside + pltpu.roll(here, nz - 1, 1)
                hpsi.append(0.5 * (6.0 * here - beside) + pot[p, pl.ds(y, 1)] * here)
                own.append(here)
                spot = (lanes == r) | (lanes == r + lane_half)
                edge = jnp.where(spot, -0.5 * pltpu.roll(here, (r + lane_half + 1) % nz, 1), edge)
            for slot, both in ((2 * group, pack(*hpsi)), (2 * group + 1, pack(*own))):
                for h in range(2):
                    high, low = parts(both[h])
                    lhs_high[h * half + k, pl.ds(slot * bands, bands)] = high
                    lhs_low[h * half + k, pl.ds(slot * bands, bands)] = low
        left_edge[group] = edge

    def accumulate(group, source, row, right_row, count):
        where = pl.ds(group * 2 * bands, 2 * bands)
        left, right = [], []
        for i in range(count):
            high, low = lhs_high[row + i, where], lhs_low[row + i, where]
            other_high, other_low = right_row(i)
            left += [high, high, low]
            right += [other_high, other_low, other_high]
        grid[source, where] += lax.dot_general(
            jnp.concatenate(left, axis=1), jnp.concatenate(right, axis=1), CONTRACT_LAST,
            preferred_element_type=jnp.float32,
        )

    def with_own(group, y, ys):
        own = pl.ds(bands, bands)
        for h in range(2):
            row = h * half + y * per_y
            accumulate(
                group, line, row, lambda i, row=row: (lhs_high[row + i, own], lhs_low[row + i, own]), ys * per_y
            )

    def with_moved(group, way, f, y, ys):
        accumulate(
            group, way.source(f), way.half_of(f) * half + y * per_y,
            lambda i: parts(way.slots[f, y * per_y + i]), ys * per_y,
        )

    def moved_all(group, f, y, ys):
        for way in ways:
            @pl.when(way.gets(f))
            def _(way=way):
                with_moved(group, way, f, y, ys)

    def take(f, t):
        for y in (2 * t, 2 * t + 1):
            for way in ways:
                @pl.when(way.gets(f))
                def _(way=way, y=y):
                    way.arrival(f, y).wait_recv()

                @pl.when(way.passes(f) & (way.shift == 0))
                def _(way=way, y=y):
                    way.hop(f, y).start()

        for way in ways:
            way.pace(f * steps + t)

    def partner_operand(y):
        for copy in forwards(y):
            copy.wait_recv()
        operand(partner, partner_halo, 1, y)

    def with_edges(group):
        into = pl.ds(2 * group * bands, bands)
        left = parts(left_edge[group])
        grid[line, into] += three(left, parts(own_edge[...]), CONTRACT_LAST, 1)
        for way in ways:
            for f in range(phases):
                @pl.when(way.gets_edge(f))
                def _(way=way, f=f):
                    keep = (low_lanes if way.base == 0 else ~low_lanes) | (way.place == 1)
                    grid[way.source(f), into] += three(
                        left, parts(jnp.where(keep, way.edges[f], 0.0)), CONTRACT_LAST, 1
                    )

    def edge_stage(f):
        for way in ways:
            @pl.when(way.gets_edge(f))
            def _(way=way):
                way.edge_arrival(f).wait_recv()

            @pl.when(way.passes(f))
            def _(way=way):
                way.edge_hop(f).start()

    def couple(group):
        for kind in range(2):
            coupled = jnp.transpose(exact(sym[kind], coef[group]))
            high, low = parts(coupled)
            where = pl.ds((2 * group + kind) * bands, bands)
            coup_high[where] = high
            coup_low[where] = low

    def project(source, right):
        grid[source] += three((coup_high[...], coup_low[...]), parts(right), MATMUL, 0)

    def coef_stage(dist):
        @pl.when(line >= dist)
        def _():
            coef_hop(dist).wait_recv()

        if dist < hops:
            @pl.when((line >= dist) & (line < last))
            def _():
                coef_hop(dist + 1).start()

        @pl.when(line >= dist)
        def _():
            project(line - dist, coef_below[dist - 1])

    def partner_row(u):
        swap(u).wait_recv()
        for copy in forwards(u):
            copy.start()

        @pl.when(u + swap_window < ny)
        def _():
            swap(u).wait_send()
            swap(u + swap_window).start()

        @pl.when(u >= 2)
        def _():
            partner_operand(u - 1)
            with_own(1, u - 1, 1)
            moved_all(1, 0, u - 1, 1)

    def first_phase(t, carry):
        for y in (halo_ahead + 2 * t, halo_ahead + 2 * t + 1):
            @pl.when(y < ny)
            def _(y=y):
                for copy in halos(y):
                    copy.start()

        for y in (2 * t, 2 * t + 1):
            for copy in halos(y):
                copy.wait_recv()
            operand(nat, halo, 0, y)
        with_own(0, 2 * t, 2)
        take(0, t)
        moved_all(0, 0, 2 * t, 2)
        partner_row(t)
        return carry

    lax.fori_loop(0, steps, first_phase, 0)

    coef_swap.wait_recv()
    couple(0)
    couple(1)
    project(line, coef[0])
    edge_stage(0)
    coef_stage(1)

    def second_phase(t, carry):
        take(1, t)
        moved_all(0, 1, 2 * t, 2)
        partner_row(steps + t)
        for y in (2 * t, 2 * t + 1):
            @pl.when((y != 0) & (y != ny - 1))
            def _(y=y):
                moved_all(1, 1, y, 1)

        for stage in range(1, hops):
            @pl.when(t == min(2 * stage, steps - 2))
            def _(stage=stage):
                if stage < phases:
                    edge_stage(stage)
                coef_stage(stage + 1)

        @pl.when(t == steps - 2)
        def _():
            with_edges(0)

        return carry

    lax.fori_loop(0, steps, second_phase, 0)
    for y in (0, ny - 1):
        partner_operand(y)
        with_own(1, y, 1)
        moved_all(1, 0, y, 1)
        moved_all(1, 1, y, 1)
    with_edges(1)
    for f in range(2, phases):
        def later_phase(t, carry, f=f):
            take(f, t)
            moved_all(0, f, 2 * t, 2)
            moved_all(1, f, 2 * t, 2)
            return carry

        lax.fori_loop(0, steps, later_phase, 0)

    if fused:
        combine(
            lines, volume, grid, result, remote, line, side, pair, dom, scratch[40:],
        )

    def finish(y, carry):
        @pl.when(y >= ny - swap_window)
        def _():
            swap(y).wait_send()

        for copy in halos(y) + forwards(y):
            copy.wait_send()
        for way in ways:
            @pl.when(way.own_first & (y < window))
            def _(way=way):
                way.sent(way.items - window + y)

            for f in range(phases):
                @pl.when(way.passes(f) & (way.shift == 0))
                def _(way=way, f=f):
                    way.hop(f, y).wait_send()

        return carry

    lax.fori_loop(0, ny, finish, 0)
    coef_swap.wait_send()
    for dist in range(1, lines):
        @pl.when((line >= dist - 1) & (line < last))
        def _(dist=dist):
            coef_hop(dist).wait_send()
    for way in ways:
        @pl.when(way.own_first)
        def _(way=way):
            way.own_edge().wait_send()

        for f in range(phases):
            @pl.when(way.passes(f))
            def _(way=way, f=f):
                way.edge_hop(f).wait_send()


def combine(lines, volume, grid, result, remote, line, side, pair, dom, scratch):
    (
        from_core, both, from_chip, total, mirror, swapped,
        core_send, core_recv, chip_send, chip_recv, line_send, line_recv, side_send, side_recv,
        near_send, near_recv, far_send, far_recv, pass_send, pass_recv,
    ) = scratch
    bands = grid.shape[2]
    core = dom % 2
    kind = dom // 2
    other_core = kind * 2 + (1 - core)
    other_chip = (1 - kind) * 2 + core
    mine = pl.ds(pl.multiple_of(core * 2 * bands, bands), 2 * bands)
    theirs = pl.ds(pl.multiple_of((1 - core) * 2 * bands, bands), 2 * bands)
    my_kind = pl.ds(pl.multiple_of(kind * bands, bands), bands)
    their_kind = pl.ds(pl.multiple_of((1 - kind) * bands, bands), bands)

    def to_core(s):
        return remote(grid.at[s, theirs], from_core.at[s], core_send.at[s], core_recv.at[s], {"dom": other_core})

    def to_chip(s):
        return remote(both.at[s, their_kind], from_chip.at[s], chip_send.at[s], chip_recv.at[s], {"dom": other_chip})

    def to_line(s):
        return remote(
            total.at[s], mirror.at[line], line_send.at[s], line_recv.at[line], {"band": s * 2 + side}
        )

    def from_line(s):
        return remote(
            total.at[s], mirror.at[s], line_send.at[s], line_recv.at[s], {"band": s * 2 + side}
        )

    def to_side(s):
        return remote(total.at[s], swapped.at[s], side_send.at[s], side_recv.at[s], {"band": pair})

    def column(s):
        block = s * 2 + jnp.where(core == 0, side, 1 - side)
        return pl.ds(pl.multiple_of(block * bands, bands), bands)

    def piece(s, k, send, recv, to):
        at = result.at[k, :, column(s)]
        return remote(at, at, send.at[s], recv.at[s], {"dom": to})

    def near(s):
        return piece(s, kind, near_send, near_recv, other_core)

    def near_arrival(s):
        block = s * 2 + jnp.where(core == 1, side, 1 - side)
        at = result.at[kind, :, pl.ds(pl.multiple_of(block * bands, bands), bands)]
        return remote(at, at, near_send.at[s], near_recv.at[s], {"dom": other_core})

    def far(s):
        return piece(s, kind, far_send, far_recv, other_chip)

    def far_arrival(s):
        return piece(s, 1 - kind, far_send, far_recv, other_chip)

    def onward(s):
        return piece(s, 1 - kind, pass_send, pass_recv, other_core)

    def onward_arrival(s):
        block = s * 2 + jnp.where(core == 1, side, 1 - side)
        at = result.at[1 - kind, :, pl.ds(pl.multiple_of(block * bands, bands), bands)]
        return remote(at, at, pass_send.at[s], pass_recv.at[s], {"dom": other_core})

    everyone = range(lines)
    for s in everyone:
        to_core(s).start()
    for s in everyone:
        to_core(s).wait_recv()
        both[s] = grid[s, mine] + from_core[s]
        to_chip(s).start()
    for s in everyone:
        to_chip(s).wait_recv()
        total[s] = both[s, my_kind] + from_chip[s]

        @pl.when(line != s)
        def _(s=s):
            to_line(s).start()

        @pl.when(core == 1)
        def _(s=s):
            to_side(s).start()
    for s in everyone:
        @pl.when(core == 1)
        def _(s=s):
            to_side(s).wait_recv()
            result[kind, :, column(s)] = volume * swapped[s]

        @pl.when(core == 0)
        def _(s=s):
            result[kind, :, column(s)] = volume * total[s]

        @pl.when(line != s)
        def _(s=s):
            from_line(s).wait_recv()
            result[kind, :, column(s)] += volume * jnp.transpose(mirror[s])

        near(s).start()
        far(s).start()
    for s in everyone:
        far_arrival(s).wait_recv()
        onward(s).start()
    for s in everyone:
        near_arrival(s).wait_recv()
        onward_arrival(s).wait_recv()
    for s in everyone:
        to_core(s).wait_send()
        to_chip(s).wait_send()
        near(s).wait_send()
        far(s).wait_send()
        onward(s).wait_send()

        @pl.when(line != s)
        def _(s=s):
            to_line(s).wait_send()

        @pl.when(core == 1)
        def _(s=s):
            to_side(s).wait_send()


def gram(psi, pot, proj, ham_corr, delta, counts, lines, doms, fused, volume):
    bands, cx, ny, nz = psi.shape
    rows = cx * ny
    half = rows // 2
    used = proj.shape[0]
    width = -(-used // 128) * 128
    hops = lines - 1
    phases = lines - 2
    f32 = jnp.float32
    dma = pltpu.SemaphoreType.DMA
    vmem = pl.BlockSpec(memory_space=pltpu.VMEM)
    hbm = pl.BlockSpec(memory_space=pl.ANY)
    scratch = [
        pltpu.VMEM((rows, bands, nz), f32),
        pltpu.VMEM((2, half, bands, nz), f32),
        pltpu.VMEM((rows, bands, nz), f32),
        pltpu.VMEM((2, ny, bands, nz), f32),
        pltpu.VMEM((2, ny, bands, nz), f32),
        pltpu.VMEM((phases, half, bands, nz), f32),
        pltpu.VMEM((phases, half, bands, nz), f32),
        pltpu.VMEM((rows, QUADS * bands, nz), jnp.bfloat16),
        pltpu.VMEM((rows, QUADS * bands, nz), jnp.bfloat16),
        pltpu.VMEM((bands, nz), f32),
        pltpu.VMEM((2, bands, nz), f32),
        pltpu.VMEM((phases, bands, nz), f32),
        pltpu.VMEM((phases, bands, nz), f32),
        pltpu.VMEM((rows, used, nz), f32),
        pltpu.VMEM((2, width, width), f32),
        pltpu.VMEM((2, width, bands), f32),
        pltpu.VMEM((hops, width, bands), f32),
        pltpu.VMEM((QUADS * bands, width), jnp.bfloat16),
        pltpu.VMEM((QUADS * bands, width), jnp.bfloat16),
        dma((rows,)), dma((rows,)), dma((ny,)), dma((ny,)), dma((2, ny)), dma((2, ny)), dma((2, ny)), dma((2, ny)),
        dma((phases, ny)), dma((phases, ny)), dma((phases, ny)), dma((phases, ny)),
        dma((phases,)), dma((phases,)), dma((phases,)), dma((phases,)),
        dma((hops,)), dma((hops,)), dma((1,)), dma((1,)),
    ]
    if fused:
        shape = (2, bands, 2 * lines * bands)
        scratch += [
            pltpu.VMEM((lines, QUADS * bands, bands), f32),
            pltpu.VMEM((lines, 2 * bands, bands), f32),
            pltpu.VMEM((lines, 2 * bands, bands), f32),
            pltpu.VMEM((lines, bands, bands), f32),
            pltpu.VMEM((lines, bands, bands), f32),
            pltpu.VMEM((lines, bands, bands), f32),
            pltpu.VMEM((lines, bands, bands), f32),
        ] + [dma((lines,))] * 14
    else:
        shape = (lines, QUADS * bands, bands)
    return pl.pallas_call(
        functools.partial(gram_kernel, lines, doms, fused, volume),
        out_shape=jax.ShapeDtypeStruct(shape, f32),
        in_specs=[pl.BlockSpec(memory_space=pltpu.SMEM), hbm, vmem, hbm, vmem, vmem],
        out_specs=vmem,
        scratch_shapes=scratch,
        compiler_params=pltpu.CompilerParams(
            collective_id=0, has_side_effects=True, vmem_limit_bytes=62 * 1024 * 1024
        ),
    )(counts, psi, pot, proj, ham_corr, delta)


def on_device(
    wavefunctions, potential, projectors, hamiltonian_correction, delta_s, projector_count
):
    bands, cx, ny, nz = wavefunctions.shape
    groups = lax.axis_size("band")
    doms = lax.axis_size("dom")
    lines = groups // 2
    mine = lax.axis_index("band")
    line, side = mine // 2, mine % 2
    volume = 1.0 / (cx * ny * nz * doms)
    atoms, slots = hamiltonian_correction.shape[:2]
    proj = projectors.reshape(atoms * slots, cx, ny, nz)
    fused = doms == QUADS and bands % 128 == 0
    grid = gram(
        wavefunctions, potential, proj, hamiltonian_correction, delta_s, projector_count,
        lines, doms, fused, volume,
    )
    if fused:
        return grid[0], grid[1]
    here = (jnp.arange(lines, dtype=jnp.int32) == line)[:, None, None, None]
    both = lax.psum(grid.reshape(lines, QUADS, bands, bands), "dom")
    lanes = [[at * 2 + s for at in range(lines)] for s in range(2)]
    mirrored = lax.all_to_all(both, "band", 0, 0, axis_index_groups=lanes, tiled=True)
    swapped = lax.ppermute(both, "band", [(i, i ^ 1) for i in range(groups)])
    crossed = (jnp.arange(QUADS, dtype=jnp.int32) >= 2)[None, :, None, None]
    total = volume * jnp.where(crossed, swapped, both) + volume * jnp.where(here, 0.0, jnp.swapaxes(mirrored, 2, 3))
    total = total.reshape(lines, 2, 2, bands, bands)
    by_side = jnp.where(side == 0, total, total[:, ::-1])
    final = jnp.transpose(by_side, (2, 3, 0, 1, 4)).reshape(2, bands, groups * bands)
    return final[0], final[1]


def solution(mesh):
    placed = (
        P("band", "dom", None, None),
        P("dom", None, None),
        P("dom", None, None, None, None),
        P("dom", None, None),
        P("dom", None, None),
        P("dom"),
    )
    return jax.shard_map(
        on_device,
        mesh=mesh,
        in_specs=placed,
        out_specs=(P("band", None), P("band", None)),
        check_vma=False,
    )
```

```python
import functools

import jax
import jax.numpy as jnp
from jax import lax
from jax.experimental import pallas as pl
from jax.experimental.pallas import tpu as pltpu
from jax.sharding import PartitionSpec as P

MESH = pl.DeviceIdType.MESH
CONTRACT_LAST = (((1,), (1,)), ((), ()))
MATMUL = (((1,), (0,)), ((), ()))
QUADS = 4
WINDOW = 8
SWAP_WINDOW = 4
HALO_AHEAD = 6


def parts(value):
    high = value.astype(jnp.bfloat16)
    low = (value - high.astype(jnp.float32)).astype(jnp.bfloat16)
    return high, low


def three(left, right, dims, axis):
    (left_high, left_low), (right_high, right_low) = left, right
    return lax.dot_general(
        jnp.concatenate([left_high, left_high, left_low], axis=1),
        jnp.concatenate([right_high, right_low, right_high], axis=axis),
        dims, preferred_element_type=jnp.float32,
    )


def exact(left, right):
    return lax.dot_general(
        left, right, MATMUL, precision=lax.Precision.HIGHEST, preferred_element_type=jnp.float32
    )


def remote(src, dst, send, recv, where):
    return pltpu.make_async_remote_copy(
        src_ref=src, dst_ref=dst, send_sem=send, recv_sem=recv,
        device_id=where, device_id_type=MESH,
    )


def gram_kernel(lines, doms, fused, volume, counts, psi_in, pot, proj_in, corrections, result, *scratch):
    (
        nat, packed, partner, halo, partner_halo, slots_r, slots_l, lhs_high, lhs_low,
        own_edge, full_edge, left_edge, edges_r, edges_l, proj, sym, coef, coef_below, coup_high, coup_low,
        load_sem, proj_sem, swap_send, swap_recv, halo_send, halo_recv, fwd_send, fwd_recv,
        right_send, right_recv, left_send, left_recv,
        right_edge_send, right_edge_recv, left_edge_send, left_edge_recv,
        coef_send, coef_recv, pair_send, pair_recv,
    ) = scratch[:40]
    rows, bands, nz = nat.shape
    cx, ny = pot.shape[:2]
    lane_half = nz // 2
    half = rows // 2
    per_y = cx // 2
    steps = ny // 2
    phases = lines - 2
    hops = lines - 1
    last = lines - 1
    window = min(WINDOW, ny)
    swap_window = min(SWAP_WINDOW, ny)
    halo_ahead = min(HALO_AHEAD, ny)
    atoms, slots = corrections.shape[1:3]
    used = atoms * slots
    live = -(-used // 8) * 8
    width = sym.shape[1]
    grid = scratch[40] if fused else result

    mine = lax.axis_index("band")
    dom = lax.axis_index("dom")
    line = mine // 2
    side = mine % 2
    pair = line * 2 + (1 - side)
    upper = jnp.minimum(line + 1, last) * 2 + side
    lower = jnp.maximum(line - 1, 0) * 2 + side
    dom_next = (dom + 1) % doms
    dom_prev = (dom + doms - 1) % doms

    def loads(y):
        copies = []
        for p in range(cx):
            r = y * cx + p
            copies.append(pltpu.make_async_copy(psi_in.at[:, p, y], nat.at[r], load_sem.at[r]))
        return copies

    def proj_loads(y):
        copies = []
        for p in range(cx):
            r = y * cx + p
            copies.append(pltpu.make_async_copy(proj_in.at[:, p, y], proj.at[r], proj_sem.at[r]))
        return copies

    def start_loads(y, carry):
        for copy in loads(y):
            copy.start()
        return carry

    def start_proj(y, carry):
        for copy in proj_loads(y):
            copy.start()
        return carry

    if fused:
        combine = Combine(lines, volume, grid, result, line, side, pair, dom, scratch[41:])
    lax.fori_loop(0, ny, start_loads, 0)
    lax.fori_loop(0, ny, start_proj, 0)

    barrier = pltpu.get_barrier_semaphore()
    pl.semaphore_signal(barrier, inc=1, device_id={"band": pair}, device_id_type=MESH)

    @pl.when(line > 0)
    def _():
        pl.semaphore_signal(barrier, inc=1, device_id={"band": lower}, device_id_type=MESH)

    @pl.when(line < last)
    def _():
        pl.semaphore_signal(barrier, inc=1, device_id={"band": upper}, device_id_type=MESH)

    for ahead in range(1, doms):
        pl.semaphore_signal(barrier, inc=1, device_id={"dom": (dom + ahead) % doms}, device_id_type=MESH)
    pl.semaphore_wait(barrier, doms + jnp.minimum(line, 1) + jnp.minimum(last - line, 1))

    def swap(y):
        at = pl.ds(y * cx, cx)
        return remote(nat.at[at], partner.at[at], swap_send.at[y], swap_recv.at[y], {"band": pair})

    def planes(src, dst, send, recv, y):
        return [
            remote(src.at[y * cx + p], dst.at[edge, y], send.at[edge, y], recv.at[edge, y], {"dom": to})
            for edge, p, to in ((0, cx - 1, dom_next), (1, 0, dom_prev))
        ]

    def halos(y):
        return planes(nat, halo, halo_send, halo_recv, y)

    def forwards(y):
        return planes(partner, partner_halo, fwd_send, fwd_recv, y)

    class Way:
        def __init__(self, base, place, slots, edges, send, recv, edge_send, edge_recv, to):
            self.base, self.place, self.slots, self.edges = base, place, slots, edges
            self.send, self.recv, self.edge_send, self.edge_recv, self.to = send, recv, edge_send, edge_recv, to
            self.count = jnp.where(place == 0, 0, jnp.where(place == 1, 2, jnp.where(place == last, last - 1, place)))
            self.own_first = place < last - 1
            self.shift = jnp.where(self.own_first, 1, 0)
            self.items = jnp.where(place == 0, 2, place + 1) * ny

        def source(self, f):
            from_place = jnp.where(
                self.place == 1, 0, jnp.where(self.place == last, self.place - 2 - f, self.place - 1 - f)
            )
            from_place = jnp.clip(from_place, 0, last)
            return from_place if self.base == 0 else last - from_place

        def half_of(self, f):
            return jnp.where(self.place == 1, 1 - self.base, self.base) if f == 1 else self.base

        def gets(self, f):
            return self.count > f

        def passes(self, f):
            return (self.place >= 1) & (self.place < last) & (self.place > f)

        def own(self, y):
            at = pl.ds(y * per_y, per_y)
            return remote(
                packed.at[self.base, at], self.slots.at[0, at], self.send.at[0, y], self.recv.at[0, y], {"band": self.to}
            )

        def extra(self, y):
            at = pl.ds(y * per_y, per_y)
            return remote(
                packed.at[1 - self.base, at], self.slots.at[1, at], self.send.at[1, y], self.recv.at[1, y],
                {"band": self.to},
            )

        def hop(self, f, y):
            at = pl.ds(y * per_y, per_y)
            q = jnp.minimum(f + self.shift, phases - 1)
            return remote(
                self.slots.at[f, at], self.slots.at[q, at], self.send.at[q, y], self.recv.at[q, y], {"band": self.to}
            )

        def arrival(self, f, y):
            at = pl.ds(y * per_y, per_y)
            return remote(
                self.slots.at[f, at], self.slots.at[f, at], self.send.at[f, y], self.recv.at[f, y], {"band": self.to}
            )

        def start_item(self, item):
            q, y = item // ny, item % ny

            @pl.when(q == 0)
            def _():
                self.own(y).start()

            @pl.when((q == 1) & (self.place == 0))
            def _():
                self.extra(y).start()

            @pl.when((q >= 1) & (self.place >= 1))
            def _():
                self.hop(jnp.clip(q - 1, 0, phases - 1), y).start()

        def sent(self, item):
            q, y = item // ny, item % ny
            at = pl.ds(y * per_y, per_y)
            remote(
                packed.at[self.base, at], self.slots.at[q, at], self.send.at[q, y], self.recv.at[q, y],
                {"band": self.to},
            ).wait_send()

        def pace(self, u):
            for item in (2 * u + window, 2 * u + window + 1):
                @pl.when(self.own_first & (item < self.items))
                def _(item=item):
                    self.sent(item - window)
                    self.start_item(item)

        def own_edge(self):
            return remote(
                own_edge.at[self.base], self.edges.at[0], self.edge_send.at[0], self.edge_recv.at[0], {"band": self.to}
            )

        def extra_edge(self):
            return remote(
                own_edge.at[1 - self.base], self.edges.at[1], self.edge_send.at[1], self.edge_recv.at[1],
                {"band": self.to},
            )

        def edge_hop(self, f):
            q = jnp.minimum(f + self.shift, phases - 1)
            return remote(
                self.edges.at[f], self.edges.at[q], self.edge_send.at[q], self.edge_recv.at[q], {"band": self.to}
            )

        def edge_arrival(self, f):
            return remote(
                self.edges.at[f], self.edges.at[f], self.edge_send.at[f], self.edge_recv.at[f], {"band": self.to}
            )

    ways = (
        Way(0, line, slots_r, edges_r, right_send, right_recv, right_edge_send, right_edge_recv, upper),
        Way(1, last - line, slots_l, edges_l, left_send, left_recv, left_edge_send, left_edge_recv, lower),
    )
    live_rows = pl.ds(0, live)
    coef_swap = remote(
        coef.at[0, live_rows], coef.at[1, live_rows], pair_send.at[0], pair_recv.at[0], {"band": pair}
    )

    def coef_hop(dist):
        src = coef.at[0, live_rows] if dist == 1 else coef_below.at[dist - 2, live_rows]
        return remote(
            src, coef_below.at[dist - 1, live_rows], coef_send.at[dist - 1], coef_recv.at[dist - 1], {"band": upper}
        )

    lanes = lax.broadcasted_iota(jnp.int32, (bands, nz), 1)
    low_lanes = lanes < lane_half

    def pack(first, second):
        low = low_lanes[: first.shape[0]]
        return (
            jnp.where(low, first, pltpu.roll(second, lane_half, 1)),
            jnp.where(low, pltpu.roll(first, lane_half, 1), second),
        )

    def start_own(y):
        for way in ways:
            @pl.when(way.own_first)
            def _(way=way):
                way.own(y).start()

    left_edge[...] = jnp.zeros_like(left_edge)

    def begin(y, carry):
        for copy in loads(y):
            copy.wait()

        @pl.when(y < swap_window)
        def _():
            swap(y).start()

        @pl.when(y < halo_ahead)
        def _():
            for copy in halos(y):
                copy.start()

        for pp in range(per_y):
            k = y * per_y + pp
            first, second = pack(nat[2 * k], nat[2 * k + 1])
            packed[0, k] = first
            packed[1, k] = second

        @pl.when((y >= 1) & (y <= window))
        def _():
            start_own(y - 1)

        return carry

    lax.fori_loop(0, ny, begin, 0)
    if window == ny:
        start_own(ny - 1)

    def gather_edge(r, carry):
        here = nat[r]
        spot = (lanes == r) | (lanes == r + lane_half)
        return jnp.where(spot, pltpu.roll(here, (r + lane_half) % nz, 1), carry)

    edge = lax.fori_loop(0, rows, gather_edge, jnp.zeros((bands, nz), jnp.float32), unroll=8)
    full_edge[...] = edge
    for h, value in enumerate(pack(edge[: bands // 2], edge[bands // 2 :])):
        own_edge[h] = value

    for kind in range(2):
        total = jnp.zeros((width, width), jnp.float32)
        for a in range(atoms):
            wide = lax.broadcasted_iota(jnp.int32, (slots, width), 0) + a * slots
            place = wide == lax.broadcasted_iota(jnp.int32, (slots, width), 1)
            place = place & (wide - a * slots < counts[a])
            tall = lax.broadcasted_iota(jnp.int32, (width, slots), 1) + a * slots
            tall_place = tall == lax.broadcasted_iota(jnp.int32, (width, slots), 0)
            tall_place = tall_place & (tall - a * slots < counts[a])
            total = total + exact(tall_place.astype(jnp.float32), exact(corrections[kind, a], place.astype(jnp.float32)))
        sym[kind] = (0.5 / volume) * (total + jnp.transpose(total))

    coef[0] = jnp.zeros((width, bands), jnp.float32)
    if live < width:
        unused = jnp.zeros((width - live, bands), jnp.float32)
        coef[1, pl.ds(live, width - live)] = unused
        for slot in range(hops):
            coef_below[slot, pl.ds(live, width - live)] = unused

    def coef_body(y, carry):
        for copy in proj_loads(y):
            copy.wait()
        left, right = [], []
        for p in range(cx):
            r = y * cx + p
            proj_high, proj_low = parts(proj[r])
            high, low = parts(nat[r])
            left += [proj_high, proj_high, proj_low]
            right += [high, low, high]
        coef[0, pl.ds(0, used)] += lax.dot_general(
            jnp.concatenate(left, axis=1), jnp.concatenate(right, axis=1), CONTRACT_LAST,
            preferred_element_type=jnp.float32,
        )
        return carry

    lax.fori_loop(0, ny, coef_body, 0)

    for way in ways:
        @pl.when(way.own_first)
        def _(way=way):
            way.own_edge().start()

        @pl.when(way.place == 0)
        def _(way=way):
            way.extra_edge().start()

    coef_swap.start()

    @pl.when(line < last)
    def _():
        coef_hop(1).start()

    grid[...] = jnp.zeros_like(grid)

    def operand(src, edges, group, y):
        up = (y + ny - 1) % ny
        down = (y + 1) % ny
        edge = left_edge[group]
        for pp in range(per_y):
            k = y * per_y + pp
            hpsi, own = [], []
            for t in range(2):
                p = 2 * pp + t
                r = y * cx + p
                here = src[r]
                before = edges[0, y] if p == 0 else src[r - 1]
                after = edges[1, y] if p == cx - 1 else src[r + 1]
                beside = before + after
                beside = beside + src[up * cx + p]
                beside = beside + src[down * cx + p]
                beside = beside + jnp.where(lanes % lane_half == 0, 0.0, pltpu.roll(here, 1, 1))
                beside = beside + pltpu.roll(here, nz - 1, 1)
                hpsi.append(0.5 * (6.0 * here - beside) + pot[p, pl.ds(y, 1)] * here)
                own.append(here)
                spot = (lanes == r) | (lanes == r + lane_half)
                edge = jnp.where(spot, -0.5 * pltpu.roll(here, (r + lane_half + 1) % nz, 1), edge)
            for slot, both in ((2 * group, pack(*hpsi)), (2 * group + 1, pack(*own))):
                for h in range(2):
                    high, low = parts(both[h])
                    lhs_high[h * half + k, pl.ds(slot * bands, bands)] = high
                    lhs_low[h * half + k, pl.ds(slot * bands, bands)] = low
        left_edge[group] = edge

    def accumulate(group, source, row, right_row, count):
        where = pl.ds(group * 2 * bands, 2 * bands)
        left, right = [], []
        for i in range(count):
            high, low = lhs_high[row + i, where], lhs_low[row + i, where]
            other_high, other_low = right_row(i)
            left += [high, high, low]
            right += [other_high, other_low, other_high]
        grid[source, where] += lax.dot_general(
            jnp.concatenate(left, axis=1), jnp.concatenate(right, axis=1), CONTRACT_LAST,
            preferred_element_type=jnp.float32,
        )

    def with_own(group, y, ys):
        own = pl.ds(bands, bands)
        for h in range(2):
            row = h * half + y * per_y
            accumulate(
                group, line, row, lambda i, row=row: (lhs_high[row + i, own], lhs_low[row + i, own]), ys * per_y
            )

    def with_moved(group, way, f, y, ys):
        accumulate(
            group, way.source(f), way.half_of(f) * half + y * per_y,
            lambda i: parts(way.slots[f, y * per_y + i]), ys * per_y,
        )

    def moved_all(group, f, y, ys):
        for way in ways:
            @pl.when(way.gets(f))
            def _(way=way):
                with_moved(group, way, f, y, ys)

    def take(f, t):
        for y in (2 * t, 2 * t + 1):
            for way in ways:
                @pl.when(way.gets(f))
                def _(way=way, y=y):
                    way.arrival(f, y).wait_recv()

                @pl.when(way.passes(f) & (way.shift == 0))
                def _(way=way, y=y):
                    way.hop(f, y).start()

        for way in ways:
            way.pace(f * steps + t)

    def partner_operand(y):
        for copy in forwards(y):
            copy.wait_recv()
        operand(partner, partner_halo, 1, y)

    def with_edges(group):
        into = pl.ds(2 * group * bands, bands)
        left = parts(left_edge[group])
        grid[line, into] += three(left, parts(full_edge[...]), CONTRACT_LAST, 1)
        for way in ways:
            for f in range(phases):
                @pl.when(way.gets(f))
                def _(way=way, f=f):
                    low = low_lanes[: bands // 2] ^ (way.half_of(f) == 1)
                    here = way.edges[f]
                    turned = pltpu.roll(here, lane_half, 1)
                    first = way.half_of(f) == 0
                    right = jnp.concatenate(
                        [
                            jnp.where(low, jnp.where(first, here, turned), 0.0),
                            jnp.where(low, jnp.where(first, turned, here), 0.0),
                        ],
                        axis=0,
                    )
                    grid[way.source(f), into] += three(left, parts(right), CONTRACT_LAST, 1)

    def edge_stage(f):
        for way in ways:
            @pl.when(way.gets(f))
            def _(way=way):
                way.edge_arrival(f).wait_recv()

            @pl.when(way.passes(f))
            def _(way=way):
                way.edge_hop(f).start()

    def couple(group):
        for kind in range(2):
            coupled = jnp.transpose(exact(sym[kind], coef[group]))
            high, low = parts(coupled)
            where = pl.ds((2 * group + kind) * bands, bands)
            coup_high[where] = high
            coup_low[where] = low

    def project(source, right):
        grid[source] += three((coup_high[...], coup_low[...]), parts(right), MATMUL, 0)

    def coef_stage(dist):
        @pl.when(line >= dist)
        def _():
            coef_hop(dist).wait_recv()

        if dist < hops:
            @pl.when((line >= dist) & (line < last))
            def _():
                coef_hop(dist + 1).start()

        @pl.when(line >= dist)
        def _():
            project(line - dist, coef_below[dist - 1])

    def partner_row(u, carry):
        swap(u).wait_recv()
        for copy in forwards(u):
            copy.start()

        @pl.when(u + swap_window < ny)
        def _():
            swap(u).wait_send()
            swap(u + swap_window).start()

        @pl.when(u >= 2)
        def _():
            partner_operand(u - 1)
            with_own(1, u - 1, 1)
            moved_all(1, 0, u - 1, 1)

        return carry

    def first_phase(t, carry):
        for y in (halo_ahead + 2 * t, halo_ahead + 2 * t + 1):
            @pl.when(y < ny)
            def _(y=y):
                for copy in halos(y):
                    copy.start()

        for y in (2 * t, 2 * t + 1):
            for copy in halos(y):
                copy.wait_recv()
            operand(nat, halo, 0, y)
        with_own(0, 2 * t, 2)
        take(0, t)
        moved_all(0, 0, 2 * t, 2)
        partner_row(t, 0)
        return carry

    lax.fori_loop(0, steps, first_phase, 0)

    coef_swap.wait_recv()
    couple(0)
    couple(1)
    project(line, coef[0])
    edge_stage(0)
    coef_stage(1)

    lead_from = steps // 2

    def second_phase(t, carry):
        take(1, t)
        moved_all(0, 1, 2 * t, 2)
        first = steps + t + jnp.where(t > lead_from, 1, 0)
        end = steps + t + 1 + jnp.where(t >= lead_from, 1, 0)
        lax.fori_loop(first, end, partner_row, 0)
        for y in (2 * t, 2 * t + 1):
            @pl.when(y != 0)
            def _(y=y):
                moved_all(1, 1, y, 1)

        for stage in range(1, hops):
            @pl.when(t == min(2 * stage, steps - 3))
            def _(stage=stage):
                if stage < phases:
                    edge_stage(stage)
                coef_stage(stage + 1)

        @pl.when(t == steps - 3)
        def _():
            with_edges(0)

        return carry

    lax.fori_loop(0, steps - 1, second_phase, 0)
    for y in (0, ny - 1):
        partner_operand(y)
        with_own(1, y, 1)
        moved_all(1, 0, y, 1)
    with_edges(1)
    take(1, steps - 1)
    moved_all(0, 1, ny - 2, 2)
    if fused and phases == 2:
        combine.send(0)
    moved_all(1, 1, ny - 2, 2)
    moved_all(1, 1, 0, 1)
    for f in range(2, phases):
        def later_phase(t, carry, f=f):
            take(f, t)
            moved_all(0, f, 2 * t, 2)
            moved_all(1, f, 2 * t, 2)
            return carry

        lax.fori_loop(0, steps, later_phase, 0)

    if fused:
        if phases > 2:
            combine.send(0)
        combine.send(1)
        combine.rest()

    def finish(y, carry):
        @pl.when(y >= ny - swap_window)
        def _():
            swap(y).wait_send()

        for copy in halos(y) + forwards(y):
            copy.wait_send()
        for way in ways:
            @pl.when(way.own_first & (y < window))
            def _(way=way):
                way.sent(way.items - window + y)

            for f in range(phases):
                @pl.when(way.passes(f) & (way.shift == 0))
                def _(way=way, f=f):
                    way.hop(f, y).wait_send()

        return carry

    lax.fori_loop(0, ny, finish, 0)
    coef_swap.wait_send()
    for dist in range(1, lines):
        @pl.when((line >= dist - 1) & (line < last))
        def _(dist=dist):
            coef_hop(dist).wait_send()
    for way in ways:
        @pl.when(way.own_first)
        def _(way=way):
            way.own_edge().wait_send()

        @pl.when(way.place == 0)
        def _(way=way):
            way.extra_edge().wait_send()

        for f in range(phases):
            @pl.when(way.passes(f))
            def _(way=way, f=f):
                way.edge_hop(f).wait_send()


class Combine:
    def __init__(self, lines, volume, grid, result, line, side, pair, dom, scratch):
        (
            from_core, both, from_chip, total, mirror, swapped,
            core_send, core_recv, chip_send, chip_recv, line_send, line_recv, side_send, side_recv,
            near_send, near_recv, far_send, far_recv, pass_send, pass_recv,
        ) = scratch
        bands = grid.shape[2]
        core = dom % 2
        kind = dom // 2
        other_core = kind * 2 + (1 - core)
        other_chip = (1 - kind) * 2 + core
        my_kind = pl.ds(pl.multiple_of(kind * bands, bands), bands)
        their_kind = pl.ds(pl.multiple_of((1 - kind) * bands, bands), bands)
        order = [(line + ahead) % lines for ahead in range(1, lines)] + [line]

        def rows(group):
            return pl.ds(group * 2 * bands, 2 * bands)

        def to_core(group, s):
            return remote(
                grid.at[s, rows(group)], from_core.at[s], core_send.at[s], core_recv.at[s], {"dom": other_core}
            )

        def to_chip(s):
            return remote(both.at[s, their_kind], from_chip.at[s], chip_send.at[s], chip_recv.at[s], {"dom": other_chip})

        def to_line(s):
            return remote(
                total.at[s], mirror.at[line], line_send.at[s], line_recv.at[line], {"band": s * 2 + side}
            )

        def from_line(s):
            return remote(
                total.at[s], mirror.at[s], line_send.at[s], line_recv.at[s], {"band": s * 2 + side}
            )

        def to_side(s):
            return remote(total.at[s], swapped.at[s], side_send.at[s], side_recv.at[s], {"band": pair})

        def piece(s, group, k, send, recv, to):
            block = s * 2 + (side if group == 0 else 1 - side)
            at = result.at[k, :, pl.ds(pl.multiple_of(block * bands, bands), bands)]
            return remote(at, at, send.at[s], recv.at[s], {"dom": to})

        def near(s, group):
            return piece(s, group, kind, near_send, near_recv, other_core)

        def far(s, group, k):
            return piece(s, group, k, far_send, far_recv, other_chip)

        def onward(s, group):
            return piece(s, group, 1 - kind, pass_send, pass_recv, other_core)

        def send(group):
            @pl.when(core == 1 - group)
            def _():
                for s in order:
                    to_core(group, s).start()

        def work(group):
            for s in order:
                to_core(group, s).wait_recv()
                both[s] = grid[s, rows(group)] + from_core[s]
                to_chip(s).start()
            for s in order:
                to_chip(s).wait_recv()
                total[s] = both[s, my_kind] + from_chip[s]
                if s is not line:
                    to_line(s).start()
                if group:
                    to_side(s).start()
            for s in order:
                if group:
                    to_side(s).wait_recv()
                    value = swapped[s]
                else:
                    value = total[s]
                if s is not line:
                    from_line(s).wait_recv()
                    value = value + jnp.transpose(mirror[s])
                block = s * 2 + (side if group == 0 else 1 - side)
                result[kind, :, pl.ds(pl.multiple_of(block * bands, bands), bands)] = volume * value
                far(s, group, kind).start()
                near(s, group).start()
            for s in order:
                far(s, group, 1 - kind).wait_recv()
                onward(s, group).start()
            for s in order:
                near(s, 1 - group).wait_recv()
                onward(s, 1 - group).wait_recv()
            for s in order:
                to_core(1 - group, s).wait_send()
                to_chip(s).wait_send()
                near(s, group).wait_send()
                far(s, group, kind).wait_send()
                onward(s, group).wait_send()
                if s is not line:
                    to_line(s).wait_send()
                if group:
                    to_side(s).wait_send()

        def rest():
            for group in range(2):
                @pl.when(core == group)
                def _(group=group):
                    work(group)

        self.send = send
        self.rest = rest


def gram(psi, pot, proj, corrections, counts, lines, doms, fused, volume):
    bands, cx, ny, nz = psi.shape
    rows = cx * ny
    half = rows // 2
    used = proj.shape[0]
    width = -(-used // 128) * 128
    hops = lines - 1
    phases = lines - 2
    f32 = jnp.float32
    dma = pltpu.SemaphoreType.DMA
    vmem = pl.BlockSpec(memory_space=pltpu.VMEM)
    hbm = pl.BlockSpec(memory_space=pl.ANY)
    scratch = [
        pltpu.VMEM((rows, bands, nz), f32),
        pltpu.VMEM((2, half, bands, nz), f32),
        pltpu.VMEM((rows, bands, nz), f32),
        pltpu.VMEM((2, ny, bands, nz), f32),
        pltpu.VMEM((2, ny, bands, nz), f32),
        pltpu.VMEM((phases, half, bands, nz), f32),
        pltpu.VMEM((phases, half, bands, nz), f32),
        pltpu.VMEM((rows, QUADS * bands, nz), jnp.bfloat16),
        pltpu.VMEM((rows, QUADS * bands, nz), jnp.bfloat16),
        pltpu.VMEM((2, bands // 2, nz), f32),
        pltpu.VMEM((bands, nz), f32),
        pltpu.VMEM((2, bands, nz), f32),
        pltpu.VMEM((phases, bands // 2, nz), f32),
        pltpu.VMEM((phases, bands // 2, nz), f32),
        pltpu.VMEM((rows, used, nz), f32),
        pltpu.VMEM((2, width, width), f32),
        pltpu.VMEM((2, width, bands), f32),
        pltpu.VMEM((hops, width, bands), f32),
        pltpu.VMEM((QUADS * bands, width), jnp.bfloat16),
        pltpu.VMEM((QUADS * bands, width), jnp.bfloat16),
        dma((rows,)), dma((rows,)), dma((ny,)), dma((ny,)), dma((2, ny)), dma((2, ny)), dma((2, ny)), dma((2, ny)),
        dma((phases, ny)), dma((phases, ny)), dma((phases, ny)), dma((phases, ny)),
        dma((phases,)), dma((phases,)), dma((phases,)), dma((phases,)),
        dma((hops,)), dma((hops,)), dma((1,)), dma((1,)),
    ]
    if fused:
        shape = (2, bands, 2 * lines * bands)
        scratch += [
            pltpu.VMEM((lines, QUADS * bands, bands), f32),
            pltpu.VMEM((lines, 2 * bands, bands), f32),
            pltpu.VMEM((lines, 2 * bands, bands), f32),
            pltpu.VMEM((lines, bands, bands), f32),
            pltpu.VMEM((lines, bands, bands), f32),
            pltpu.VMEM((lines, bands, bands), f32),
            pltpu.VMEM((lines, bands, bands), f32),
        ] + [dma((lines,))] * 14
    else:
        shape = (lines, QUADS * bands, bands)
    return pl.pallas_call(
        functools.partial(gram_kernel, lines, doms, fused, volume),
        out_shape=jax.ShapeDtypeStruct(shape, f32),
        in_specs=[pl.BlockSpec(memory_space=pltpu.SMEM), hbm, vmem, hbm, vmem],
        out_specs=vmem,
        scratch_shapes=scratch,
        compiler_params=pltpu.CompilerParams(
            collective_id=0, has_side_effects=True, vmem_limit_bytes=62 * 1024 * 1024
        ),
    )(counts, psi, pot, proj, corrections)


def on_device(
    wavefunctions, potential, projectors, hamiltonian_correction, delta_s, projector_count
):
    bands, cx, ny, nz = wavefunctions.shape
    groups = lax.axis_size("band")
    doms = lax.axis_size("dom")
    lines = groups // 2
    mine = lax.axis_index("band")
    line, side = mine // 2, mine % 2
    volume = 1.0 / (cx * ny * nz * doms)
    atoms, slots = hamiltonian_correction.shape[:2]
    proj = projectors.reshape(atoms * slots, cx, ny, nz)
    fused = doms == QUADS and bands % 128 == 0
    grid = gram(
        wavefunctions, potential, proj, jnp.stack([hamiltonian_correction, delta_s]), projector_count,
        lines, doms, fused, volume,
    )
    if fused:
        return grid[0], grid[1]
    here = (jnp.arange(lines, dtype=jnp.int32) == line)[:, None, None, None]
    both = lax.psum(grid.reshape(lines, QUADS, bands, bands), "dom")
    lanes = [[at * 2 + s for at in range(lines)] for s in range(2)]
    mirrored = lax.all_to_all(both, "band", 0, 0, axis_index_groups=lanes, tiled=True)
    swapped = lax.ppermute(both, "band", [(i, i ^ 1) for i in range(groups)])
    crossed = (jnp.arange(QUADS, dtype=jnp.int32) >= 2)[None, :, None, None]
    total = volume * jnp.where(crossed, swapped, both) + volume * jnp.where(here, 0.0, jnp.swapaxes(mirrored, 2, 3))
    total = total.reshape(lines, 2, 2, bands, bands)
    by_side = jnp.where(side == 0, total, total[:, ::-1])
    final = jnp.transpose(by_side, (2, 3, 0, 1, 4)).reshape(2, bands, groups * bands)
    return final[0], final[1]


def solution(mesh):
    placed = (
        P("band", "dom", None, None),
        P("dom", None, None),
        P("dom", None, None, None, None),
        P("dom", None, None),
        P("dom", None, None),
        P("dom"),
    )
    return jax.shard_map(
        on_device,
        mesh=mesh,
        in_specs=placed,
        out_specs=(P("band", None), P("band", None)),
        check_vma=False,
    )
```

```python
import functools

import jax
import jax.numpy as jnp
from jax import lax
from jax.experimental import pallas as pl
from jax.experimental.pallas import tpu as pltpu
from jax.sharding import PartitionSpec as P

MESH = pl.DeviceIdType.MESH
CONTRACT_LAST = (((1,), (1,)), ((), ()))
MATMUL = (((1,), (0,)), ((), ()))
QUADS = 4
WINDOW = 4
SWAP_WINDOW = 3
HALO_AHEAD = 6


def parts(value):
    high = value.astype(jnp.bfloat16)
    low = (value - high.astype(jnp.float32)).astype(jnp.bfloat16)
    return high, low


def three(left, right, dims, axis):
    (left_high, left_low), (right_high, right_low) = left, right
    return lax.dot_general(
        jnp.concatenate([left_high, left_high, left_low], axis=1),
        jnp.concatenate([right_high, right_low, right_high], axis=axis),
        dims, preferred_element_type=jnp.float32,
    )


def exact(left, right):
    return lax.dot_general(
        left, right, MATMUL, precision=lax.Precision.HIGHEST, preferred_element_type=jnp.float32
    )


def remote(src, dst, send, recv, where):
    return pltpu.make_async_remote_copy(
        src_ref=src, dst_ref=dst, send_sem=send, recv_sem=recv,
        device_id=where, device_id_type=MESH,
    )


def gram_kernel(lines, doms, fused, volume, counts, psi_in, pot, proj_in, ham_corr, delta, *scratch):
    result, scratch = scratch[0], scratch[1:]
    (
        nat, packed, partner, halo, partner_halo, slots_r, slots_l, lhs_high, lhs_low,
        own_edge, full_edge, left_edge, edges_r, edges_l, proj, sym, coef, coef_below, coup_high, coup_low,
        load_sem, proj_sem, swap_send, swap_recv, halo_send, halo_recv, fwd_send, fwd_recv,
        right_send, right_recv, left_send, left_recv,
        right_edge_send, right_edge_recv, left_edge_send, left_edge_recv,
        coef_send, coef_recv, pair_send, pair_recv,
    ) = scratch[:40]
    rows, bands, nz = nat.shape
    cx, ny = pot.shape[:2]
    lane_half = nz // 2
    half = rows // 2
    per_y = cx // 2
    steps = ny // 2
    phases = lines - 2
    hops = lines - 1
    last = lines - 1
    window = min(WINDOW, ny)
    swap_window = min(SWAP_WINDOW, ny)
    halo_ahead = min(HALO_AHEAD, ny)
    slots, atoms = ham_corr.shape[:2]
    used = atoms * slots
    live = -(-used // 8) * 8
    width = sym.shape[1]
    grid = scratch[40] if fused else result

    mine = lax.axis_index("band")
    dom = lax.axis_index("dom")
    line = mine // 2
    side = mine % 2
    pair = line * 2 + (1 - side)
    upper = jnp.minimum(line + 1, last) * 2 + side
    lower = jnp.maximum(line - 1, 0) * 2 + side
    dom_next = (dom + 1) % doms
    dom_prev = (dom + doms - 1) % doms

    def loads(y):
        copies = []
        for p in range(cx):
            r = y * cx + p
            copies.append(pltpu.make_async_copy(psi_in.at[:, p, y], nat.at[r], load_sem.at[y]))
        return copies

    def proj_loads(y):
        copies = []
        for p in range(cx):
            r = y * cx + p
            copies.append(pltpu.make_async_copy(proj_in.at[:, p, y], proj.at[r], proj_sem.at[0]))
        return copies

    def start_loads(y, carry):
        for copy in loads(y):
            copy.start()
        return carry

    def start_proj(y, carry):
        for copy in proj_loads(y):
            copy.start()
        return carry

    if fused:
        combine = Combine(lines, volume, grid, result, line, side, pair, dom, scratch[41:])
    lax.fori_loop(0, ny, start_loads, 0)
    lax.fori_loop(0, ny, start_proj, 0)

    barrier = pltpu.get_barrier_semaphore()
    pl.semaphore_signal(barrier, inc=1, device_id={"band": pair}, device_id_type=MESH)

    @pl.when(line > 0)
    def _():
        pl.semaphore_signal(barrier, inc=1, device_id={"band": lower}, device_id_type=MESH)

    @pl.when(line < last)
    def _():
        pl.semaphore_signal(barrier, inc=1, device_id={"band": upper}, device_id_type=MESH)

    for ahead in range(1, doms):
        pl.semaphore_signal(barrier, inc=1, device_id={"dom": (dom + ahead) % doms}, device_id_type=MESH)
    pl.semaphore_wait(barrier, doms + jnp.minimum(line, 1) + jnp.minimum(last - line, 1))

    def swap(y):
        at = pl.ds(y * cx, cx)
        return remote(nat.at[at], partner.at[at], swap_send.at[y % swap_window], swap_recv.at[y], {"band": pair})

    def planes(src, dst, send, recv, y):
        return [
            remote(src.at[y * cx + p], dst.at[edge, y], send.at[0], recv.at[y], {"dom": to})
            for edge, p, to in ((0, cx - 1, dom_next), (1, 0, dom_prev))
        ]

    def both_planes(dst, send, recv, y):
        return remote(dst.at[:, y], dst.at[:, y], send.at[0], recv.at[y], {"dom": dom_next})

    def halos(y):
        return planes(nat, halo, halo_send, halo_recv, y)

    def forwards(y):
        return planes(partner, partner_halo, fwd_send, fwd_recv, y)

    class Way:
        def __init__(self, base, place, slots, edges, send, recv, edge_send, edge_recv, to):
            self.base, self.place, self.slots, self.edges = base, place, slots, edges
            self.send, self.recv, self.edge_send, self.edge_recv, self.to = send, recv, edge_send, edge_recv, to
            self.count = jnp.where(place == 0, 0, jnp.where(place == 1, 2, jnp.where(place == last, last - 1, place)))
            self.own_first = place < last - 1
            self.shift = jnp.where(self.own_first, 1, 0)
            self.items = jnp.where(place == 0, 2, place + 1) * ny

        def source(self, f):
            from_place = jnp.where(
                self.place == 1, 0, jnp.where(self.place == last, self.place - 2 - f, self.place - 1 - f)
            )
            from_place = jnp.clip(from_place, 0, last)
            return from_place if self.base == 0 else last - from_place

        def half_of(self, f):
            return jnp.where(self.place == 1, 1 - self.base, self.base) if f == 1 else self.base

        def gets(self, f):
            return self.count > f

        def passes(self, f):
            return (self.place >= 1) & (self.place < last) & (self.place > f)

        def own(self, y):
            at = pl.ds(y * per_y, per_y)
            return remote(
                packed.at[self.base, at], self.slots.at[0, at], self.send.at[y % window], self.recv.at[0, y],
                {"band": self.to},
            )

        def extra(self, y):
            at = pl.ds(y * per_y, per_y)
            return remote(
                packed.at[1 - self.base, at], self.slots.at[1, at], self.send.at[(ny + y) % window], self.recv.at[1, y],
                {"band": self.to},
            )

        def hop(self, f, y):
            at = pl.ds(y * per_y, per_y)
            q = jnp.minimum(f + self.shift, phases - 1)
            slot = jnp.where(self.own_first, (q * ny + y) % window, window)
            return remote(
                self.slots.at[f, at], self.slots.at[q, at], self.send.at[slot], self.recv.at[q, y], {"band": self.to}
            )

        def arrival(self, f, y):
            at = pl.ds(y * per_y, per_y)
            return remote(
                self.slots.at[f, at], self.slots.at[f, at], self.send.at[0], self.recv.at[f, y], {"band": self.to}
            )

        def start_item(self, item):
            q, y = item // ny, item % ny

            @pl.when(q == 0)
            def _():
                self.own(y).start()

            @pl.when((q == 1) & (self.place == 0))
            def _():
                self.extra(y).start()

            @pl.when((q >= 1) & (self.place >= 1))
            def _():
                self.hop(jnp.clip(q - 1, 0, phases - 1), y).start()

        def sent(self, item):
            q, y = item // ny, item % ny
            at = pl.ds(y * per_y, per_y)
            remote(
                packed.at[self.base, at], self.slots.at[q, at], self.send.at[item % window], self.recv.at[q, y],
                {"band": self.to},
            ).wait_send()

        def pace(self, item):
            @pl.when(self.own_first & (item < self.items))
            def _():
                self.sent(item - window)
                self.start_item(item)

        def own_edge(self):
            return remote(
                own_edge.at[self.base], self.edges.at[0], self.edge_send.at[0], self.edge_recv.at[0], {"band": self.to}
            )

        def extra_edge(self):
            return remote(
                own_edge.at[1 - self.base], self.edges.at[1], self.edge_send.at[1], self.edge_recv.at[1],
                {"band": self.to},
            )

        def edge_hop(self, f):
            q = jnp.minimum(f + self.shift, phases - 1)
            return remote(
                self.edges.at[f], self.edges.at[q], self.edge_send.at[q], self.edge_recv.at[q], {"band": self.to}
            )

        def edge_arrival(self, f):
            return remote(
                self.edges.at[f], self.edges.at[f], self.edge_send.at[f], self.edge_recv.at[f], {"band": self.to}
            )

    ways = (
        Way(0, line, slots_r, edges_r, right_send, right_recv, right_edge_send, right_edge_recv, upper),
        Way(1, last - line, slots_l, edges_l, left_send, left_recv, left_edge_send, left_edge_recv, lower),
    )
    live_rows = pl.ds(0, live)
    coef_swap = remote(
        coef.at[0, live_rows], coef.at[1, live_rows], pair_send.at[0], pair_recv.at[0], {"band": pair}
    )

    def coef_hop(dist):
        src = coef.at[0, live_rows] if dist == 1 else coef_below.at[dist - 2, live_rows]
        return remote(
            src, coef_below.at[dist - 1, live_rows], coef_send.at[dist - 1], coef_recv.at[dist - 1], {"band": upper}
        )

    lanes = lax.broadcasted_iota(jnp.int32, (bands, nz), 1)
    low_lanes = lanes < lane_half

    def pack(first, second):
        low = low_lanes[: first.shape[0]]
        return (
            jnp.where(low, first, pltpu.roll(second, lane_half, 1)),
            jnp.where(low, pltpu.roll(first, lane_half, 1), second),
        )

    def take(f, y):
        for way in ways:
            @pl.when(way.gets(f))
            def _(way=way):
                way.arrival(f, y).wait_recv()

            @pl.when(way.passes(f) & (way.shift == 0))
            def _(way=way):
                way.hop(f, y).start()

        for way in ways:
            way.pace(f * ny + y + window)

    def start_own(y):
        for way in ways:
            @pl.when(way.own_first)
            def _(way=way):
                way.own(y).start()

    left_edge[...] = jnp.zeros_like(left_edge)

    def begin(y, carry):
        at = pl.ds(y * cx, cx)
        pltpu.make_async_copy(nat.at[at], nat.at[at], load_sem.at[y]).wait()

        @pl.when(y < swap_window)
        def _():
            swap(y).start()

        @pl.when(y < halo_ahead)
        def _():
            for copy in halos(y):
                copy.start()

        for pp in range(per_y):
            k = y * per_y + pp
            first, second = pack(nat[2 * k], nat[2 * k + 1])
            packed[0, k] = first
            packed[1, k] = second

        @pl.when((y >= 1) & (y <= window))
        def _():
            start_own(y - 1)

        return carry

    lax.fori_loop(0, ny, begin, 0)
    if window == ny:
        start_own(ny - 1)

    def gather_edge(r, carry):
        here = nat[r]
        spot = (lanes == r) | (lanes == r + lane_half)
        return jnp.where(spot, pltpu.roll(here, (r + lane_half) % nz, 1), carry)

    edge = lax.fori_loop(0, rows, gather_edge, jnp.zeros((bands, nz), jnp.float32), unroll=8)
    full_edge[...] = edge
    for h, value in enumerate(pack(edge[: bands // 2], edge[bands // 2 :])):
        own_edge[h] = value

    take(0, 0)
    for kind, source in enumerate((ham_corr, delta)):
        total = jnp.zeros((width, width), jnp.float32)
        for a in range(atoms):
            wide = lax.broadcasted_iota(jnp.int32, (slots, width), 0) + a * slots
            place = wide == lax.broadcasted_iota(jnp.int32, (slots, width), 1)
            place = place & (wide - a * slots < counts[a])
            tall = lax.broadcasted_iota(jnp.int32, (width, slots), 1) + a * slots
            tall_place = tall == lax.broadcasted_iota(jnp.int32, (width, slots), 0)
            tall_place = tall_place & (tall - a * slots < counts[a])
            total = total + exact(tall_place.astype(jnp.float32), exact(source[:, a], place.astype(jnp.float32)))
        sym[kind] = (0.5 / volume) * (total + jnp.transpose(total))

    coef[0] = jnp.zeros((width, bands), jnp.float32)
    if live < width:
        unused = jnp.zeros((width - live, bands), jnp.float32)
        coef[1, pl.ds(live, width - live)] = unused
        for slot in range(hops):
            coef_below[slot, pl.ds(live, width - live)] = unused

    def coef_body(y, carry):
        left, right = [], []
        for p in range(cx):
            r = y * cx + p
            proj_high, proj_low = parts(proj[r])
            high, low = parts(nat[r])
            left += [proj_high, proj_high, proj_low]
            right += [high, low, high]
        coef[0, pl.ds(0, used)] += lax.dot_general(
            jnp.concatenate(left, axis=1), jnp.concatenate(right, axis=1), CONTRACT_LAST,
            preferred_element_type=jnp.float32,
        )
        return carry

    pltpu.make_async_copy(proj, proj, proj_sem.at[0]).wait()
    lax.fori_loop(0, ny // 2, coef_body, 0)
    take(0, 1)
    lax.fori_loop(ny // 2, ny, coef_body, 0)
    take(0, 2)

    for way in ways:
        @pl.when(way.own_first)
        def _(way=way):
            way.own_edge().start()

        @pl.when(way.place == 0)
        def _(way=way):
            way.extra_edge().start()

    coef_swap.start()

    @pl.when(line < last)
    def _():
        coef_hop(1).start()

    grid[...] = jnp.zeros_like(grid)

    def operand(src, edges, group, y):
        up = (y + ny - 1) % ny
        down = (y + 1) % ny
        edge = left_edge[group]
        for pp in range(per_y):
            k = y * per_y + pp
            hpsi, own = [], []
            for t in range(2):
                p = 2 * pp + t
                r = y * cx + p
                here = src[r]
                before = edges[0, y] if p == 0 else src[r - 1]
                after = edges[1, y] if p == cx - 1 else src[r + 1]
                beside = before + after
                beside = beside + src[up * cx + p]
                beside = beside + src[down * cx + p]
                beside = beside + jnp.where(lanes % lane_half == 0, 0.0, pltpu.roll(here, 1, 1))
                beside = beside + pltpu.roll(here, nz - 1, 1)
                hpsi.append(0.5 * (6.0 * here - beside) + pot[p, pl.ds(y, 1)] * here)
                own.append(here)
                spot = (lanes == r) | (lanes == r + lane_half)
                edge = jnp.where(spot, -0.5 * pltpu.roll(here, (r + lane_half + 1) % nz, 1), edge)
            for slot, both in ((2 * group, pack(*hpsi)), (2 * group + 1, pack(*own))):
                for h in range(2):
                    high, low = parts(both[h])
                    lhs_high[h * half + k, pl.ds(slot * bands, bands)] = high
                    lhs_low[h * half + k, pl.ds(slot * bands, bands)] = low
        left_edge[group] = edge

    def accumulate(group, source, row, right_row, count):
        where = pl.ds(group * 2 * bands, 2 * bands)
        left, right = [], []
        for i in range(count):
            high, low = lhs_high[row + i, where], lhs_low[row + i, where]
            other_high, other_low = right_row(i)
            left += [high, high, low]
            right += [other_high, other_low, other_high]
        grid[source, where] += lax.dot_general(
            jnp.concatenate(left, axis=1), jnp.concatenate(right, axis=1), CONTRACT_LAST,
            preferred_element_type=jnp.float32,
        )

    def with_own(group, y, ys):
        own = pl.ds(bands, bands)
        for h in range(2):
            row = h * half + y * per_y
            accumulate(
                group, line, row, lambda i, row=row: (lhs_high[row + i, own], lhs_low[row + i, own]), ys * per_y
            )

    def with_moved(group, way, f, y, ys):
        accumulate(
            group, way.source(f), way.half_of(f) * half + y * per_y,
            lambda i: parts(way.slots[f, y * per_y + i]), ys * per_y,
        )

    def moved_all(group, f, y, ys):
        for way in ways:
            @pl.when(way.gets(f))
            def _(way=way):
                with_moved(group, way, f, y, ys)

    def partner_operand(y):
        both_planes(partner_halo, fwd_send, fwd_recv, y).wait_recv()
        operand(partner, partner_halo, 1, y)

    def with_edges(group):
        into = pl.ds(2 * group * bands, bands)
        low = low_lanes[: bands // 2]
        right = [full_edge[...]]
        found = []
        for way in ways:
            for f in range(phases):
                here = way.edges[f]
                turned = pltpu.roll(here, lane_half, 1)
                first = way.half_of(f) == 0
                keep = (low ^ (way.half_of(f) == 1)) & way.gets(f)
                right.append(jnp.where(keep, jnp.where(first, here, turned), 0.0))
                right.append(jnp.where(keep, jnp.where(first, turned, here), 0.0))
                found.append((way, f))
        added = three(parts(left_edge[group]), parts(jnp.concatenate(right, axis=0)), CONTRACT_LAST, 1)
        grid[line, into] += added[:, :bands]
        for at, (way, f) in enumerate(found):
            @pl.when(way.gets(f))
            def _(way=way, f=f, at=at):
                grid[way.source(f), into] += added[:, (at + 1) * bands : (at + 2) * bands]

    def edge_stage(f):
        for way in ways:
            @pl.when(way.gets(f))
            def _(way=way):
                way.edge_arrival(f).wait_recv()

            @pl.when(way.passes(f))
            def _(way=way):
                way.edge_hop(f).start()

    def couple(group):
        for kind in range(2):
            coupled = jnp.transpose(exact(sym[kind], coef[group]))
            high, low = parts(coupled)
            where = pl.ds((2 * group + kind) * bands, bands)
            coup_high[where] = high
            coup_low[where] = low

    def project(source, right):
        grid[source] += three((coup_high[...], coup_low[...]), parts(right), MATMUL, 0)

    def coef_stage(dist):
        @pl.when(line >= dist)
        def _():
            coef_hop(dist).wait_recv()

        if dist < hops:
            @pl.when((line >= dist) & (line < last))
            def _():
                coef_hop(dist + 1).start()

        @pl.when(line >= dist)
        def _():
            project(line - dist, coef_below[dist - 1])

    def partner_row(u, carry):
        swap(u).wait_recv()
        for copy in forwards(u):
            copy.start()

        @pl.when(u + swap_window < ny)
        def _():
            swap(u).wait_send()
            swap(u + swap_window).start()

        @pl.when(u >= 2)
        def _():
            partner_operand(u - 1)
            with_own(1, u - 1, 1)
            moved_all(1, 0, u - 1, 1)

        return carry

    def first_phase(t, carry):
        for y in (halo_ahead + 2 * t, halo_ahead + 2 * t + 1):
            @pl.when(y < ny)
            def _(y=y):
                for copy in halos(y):
                    copy.start()

        @pl.when(t >= 2)
        def _():
            take(0, 2 * t)

        for y in (2 * t, 2 * t + 1):
            both_planes(halo, halo_send, halo_recv, y).wait_recv()
            operand(nat, halo, 0, y)
        with_own(0, 2 * t, 2)

        @pl.when(t >= 2)
        def _():
            take(0, 2 * t + 1)

        @pl.when(t == 0)
        def _():
            take(0, 3)

        moved_all(0, 0, 2 * t, 2)
        partner_row(t, 0)
        return carry

    lax.fori_loop(0, steps, first_phase, 0)

    coef_swap.wait_recv()
    couple(0)
    couple(1)
    project(line, coef[0])
    edge_stage(0)
    coef_stage(1)

    def second_phase(t, carry):
        take(1, 2 * t)
        partner_row(steps + t, 0)
        take(1, 2 * t + 1)
        moved_all(0, 1, 2 * t, 2)
        for y in (2 * t, 2 * t + 1):
            @pl.when(y != 0)
            def _(y=y):
                moved_all(1, 1, y, 1)

        for stage in range(1, hops):
            @pl.when(t == min(2 * stage + 1, steps - 3))
            def _(stage=stage):
                if stage < phases:
                    edge_stage(stage)
                coef_stage(stage + 1)

        @pl.when(t == steps - 3)
        def _():
            with_edges(0)

        return carry

    lax.fori_loop(0, steps - 1, second_phase, 0)
    take(1, ny - 2)
    partner_row(ny - 1, 0)
    partner_operand(0)
    with_own(1, 0, 1)
    moved_all(1, 0, 0, 1)
    moved_all(1, 1, 0, 1)
    take(1, ny - 1)
    moved_all(0, 1, ny - 2, 2)
    early = fused and phases == 2
    if early:
        combine.send(0)
    partner_operand(ny - 1)
    with_own(1, ny - 1, 1)
    moved_all(1, 0, ny - 1, 1)
    if early:
        combine.reduce(0)
    moved_all(1, 1, ny - 2, 2)
    with_edges(1)
    for f in range(2, phases):
        def later_phase(t, carry, f=f):
            take(f, 2 * t)
            take(f, 2 * t + 1)
            moved_all(0, f, 2 * t, 2)
            moved_all(1, f, 2 * t, 2)
            return carry

        lax.fori_loop(0, steps, later_phase, 0)

    if fused:
        if not early:
            combine.send(0)
            combine.reduce(0)
        combine.send(1)
        combine.reduce(1)
        combine.rest()

    for y in range(ny - swap_window, ny):
        swap(y).wait_send()
    remote(halo, halo, halo_send.at[0], halo_recv.at[0], {"dom": dom_next}).wait_send()
    remote(partner_halo, partner_halo, fwd_send.at[0], fwd_recv.at[0], {"dom": dom_next}).wait_send()
    for way in ways:
        @pl.when(way.own_first)
        def _(way=way):
            for ahead in range(window):
                way.sent(way.items - window + ahead)

        @pl.when(way.place == last - 1)
        def _(way=way):
            remote(
                way.slots, way.slots, way.send.at[window], way.recv.at[0, 0], {"band": way.to}
            ).wait_send()

    coef_swap.wait_send()
    for dist in range(1, lines):
        @pl.when((line >= dist - 1) & (line < last))
        def _(dist=dist):
            coef_hop(dist).wait_send()
    for way in ways:
        @pl.when(way.own_first)
        def _(way=way):
            way.own_edge().wait_send()

        @pl.when(way.place == 0)
        def _(way=way):
            way.extra_edge().wait_send()

        for f in range(phases):
            @pl.when(way.passes(f))
            def _(way=way, f=f):
                way.edge_hop(f).wait_send()


class Combine:
    def __init__(self, lines, volume, grid, out, line, side, pair, dom, scratch):
        (
            from_core, both, from_chip, total, mirror, swapped,
            core_send, core_recv, chip_send, chip_recv, line_send, line_recv, side_send, side_recv,
            near_send, near_recv, far_send, far_recv, pass_send, pass_recv, result, out_sem,
        ) = scratch
        bands = grid.shape[2]
        core = dom % 2
        kind = dom // 2
        other_core = kind * 2 + (1 - core)
        other_chip = (1 - kind) * 2 + core
        my_kind = pl.ds(pl.multiple_of(kind * bands, bands), bands)
        their_kind = pl.ds(pl.multiple_of((1 - kind) * bands, bands), bands)
        order = [(line + ahead) % lines for ahead in range(1, lines)] + [line]

        def rows(group):
            return pl.ds(group * 2 * bands, 2 * bands)

        def to_core(group, s):
            return remote(
                grid.at[s, rows(group)], from_core.at[s], core_send.at[0], core_recv.at[s], {"dom": other_core}
            )

        def to_chip(s):
            return remote(both.at[s, their_kind], from_chip.at[s], chip_send.at[0], chip_recv.at[s], {"dom": other_chip})

        def to_line(s):
            return remote(
                total.at[s], mirror.at[line], line_send.at[0], line_recv.at[line], {"band": s * 2 + side}
            )

        def from_line(s):
            return remote(
                total.at[s], mirror.at[s], line_send.at[0], line_recv.at[s], {"band": s * 2 + side}
            )

        def to_side(s):
            return remote(total.at[s], swapped.at[s], side_send.at[0], side_recv.at[s], {"band": pair})

        def piece(s, group, k, send, recv, to):
            block = s * 2 + (side if group == 0 else 1 - side)
            at = result.at[k, :, pl.ds(pl.multiple_of(block * bands, bands), bands)]
            return remote(at, at, send.at[0], recv.at[s], {"dom": to})

        def near(s, group):
            return piece(s, group, kind, near_send, near_recv, other_core)

        def far(s, group, k):
            return piece(s, group, k, far_send, far_recv, other_chip)

        def onward(s, group):
            return piece(s, group, 1 - kind, pass_send, pass_recv, other_core)

        def send(group):
            @pl.when(core == 1 - group)
            def _():
                for s in order:
                    to_core(group, s).start()

        def flush(s, group, k):
            block = s * 2 + (side if group == 0 else 1 - side)
            at = (k, slice(None), pl.ds(pl.multiple_of(block * bands, bands), bands))
            pltpu.make_async_copy(result.at[at], out.at[at], out_sem.at[0]).start()

        def reduce(group):
            @pl.when(core == group)
            def _():
                for s in order:
                    to_core(group, s).wait_recv()
                    both[s] = grid[s, rows(group)] + from_core[s]
                    to_chip(s).start()

        def work(group):
            for s in order:
                to_chip(s).wait_recv()
                total[s] = both[s, my_kind] + from_chip[s]
                if s is not line:
                    to_line(s).start()
                if group:
                    to_side(s).start()
            for s in order:
                if group:
                    to_side(s).wait_recv()
                    value = swapped[s]
                else:
                    value = total[s]
                if s is not line:
                    from_line(s).wait_recv()
                    value = value + jnp.transpose(mirror[s])
                block = s * 2 + (side if group == 0 else 1 - side)
                result[kind, :, pl.ds(pl.multiple_of(block * bands, bands), bands)] = volume * value
                far(s, group, kind).start()
                near(s, group).start()
                flush(s, group, kind)
            for s in order:
                near(s, 1 - group).wait_recv()
                flush(s, 1 - group, kind)
            for s in order:
                far(s, group, 1 - kind).wait_recv()
                onward(s, group).start()
                flush(s, group, 1 - kind)
            for s in order:
                onward(s, 1 - group).wait_recv()
                flush(s, 1 - group, 1 - kind)
            pltpu.make_async_copy(result, result, out_sem.at[0]).wait()
            for held, send, recv in (
                (from_core, core_send, core_recv), (from_chip, chip_send, chip_recv),
                (mirror.at[pl.ds(0, lines - 1)], line_send, line_recv), (total, near_send, near_recv),
                (total, far_send, far_recv), (total, pass_send, pass_recv),
            ):
                remote(held, held, send.at[0], recv.at[0], {"dom": other_core}).wait_send()
            if group:
                remote(swapped, swapped, side_send.at[0], side_recv.at[0], {"dom": other_core}).wait_send()

        def rest():
            for group in range(2):
                @pl.when(core == group)
                def _(group=group):
                    work(group)

        self.send = send
        self.reduce = reduce
        self.rest = rest


def gram(psi, pot, proj, ham_corr, delta, counts, lines, doms, fused, volume):
    bands, cx, ny, nz = psi.shape
    rows = cx * ny
    half = rows // 2
    used = proj.shape[0]
    width = -(-used // 128) * 128
    hops = lines - 1
    phases = lines - 2
    window = min(WINDOW, ny) + 1
    f32 = jnp.float32
    dma = pltpu.SemaphoreType.DMA
    vmem = pl.BlockSpec(memory_space=pltpu.VMEM)
    hbm = pl.BlockSpec(memory_space=pl.ANY)
    scratch = [
        pltpu.VMEM((rows, bands, nz), f32),
        pltpu.VMEM((2, half, bands, nz), f32),
        pltpu.VMEM((rows, bands, nz), f32),
        pltpu.VMEM((2, ny, bands, nz), f32),
        pltpu.VMEM((2, ny, bands, nz), f32),
        pltpu.VMEM((phases, half, bands, nz), f32),
        pltpu.VMEM((phases, half, bands, nz), f32),
        pltpu.VMEM((rows, QUADS * bands, nz), jnp.bfloat16),
        pltpu.VMEM((rows, QUADS * bands, nz), jnp.bfloat16),
        pltpu.VMEM((2, bands // 2, nz), f32),
        pltpu.VMEM((bands, nz), f32),
        pltpu.VMEM((2, bands, nz), f32),
        pltpu.VMEM((phases, bands // 2, nz), f32),
        pltpu.VMEM((phases, bands // 2, nz), f32),
        pltpu.VMEM((rows, used, nz), f32),
        pltpu.VMEM((2, width, width), f32),
        pltpu.VMEM((2, width, bands), f32),
        pltpu.VMEM((hops, width, bands), f32),
        pltpu.VMEM((QUADS * bands, width), jnp.bfloat16),
        pltpu.VMEM((QUADS * bands, width), jnp.bfloat16),
        dma((ny,)), dma((1,)), dma((min(SWAP_WINDOW, ny),)), dma((ny,)), dma((1,)), dma((ny,)), dma((1,)), dma((ny,)),
        dma((window,)), dma((phases, ny)), dma((window,)), dma((phases, ny)),
        dma((phases,)), dma((phases,)), dma((phases,)), dma((phases,)),
        dma((hops,)), dma((hops,)), dma((1,)), dma((1,)),
    ]
    if fused:
        columns = 2 * lines * bands
        shape = jax.ShapeDtypeStruct((2, bands, columns), f32)
        placed = hbm
        scratch += [
            pltpu.VMEM((lines, QUADS * bands, bands), f32),
            pltpu.VMEM((lines, 2 * bands, bands), f32),
            pltpu.VMEM((lines, 2 * bands, bands), f32),
            pltpu.VMEM((lines, bands, bands), f32),
            pltpu.VMEM((lines, bands, bands), f32),
            pltpu.VMEM((lines, bands, bands), f32),
            pltpu.VMEM((lines, bands, bands), f32),
        ] + [dma((1,)), dma((lines,))] * 7 + [pltpu.VMEM((2, bands, columns), f32), dma((1,))]
    else:
        shape = jax.ShapeDtypeStruct((lines, QUADS * bands, bands), f32)
        placed = vmem
    return pl.pallas_call(
        functools.partial(gram_kernel, lines, doms, fused, volume),
        out_shape=shape,
        in_specs=[pl.BlockSpec(memory_space=pltpu.SMEM), hbm, vmem, hbm, vmem, vmem],
        out_specs=placed,
        scratch_shapes=scratch,
        compiler_params=pltpu.CompilerParams(
            collective_id=0, has_side_effects=True, vmem_limit_bytes=62 * 1024 * 1024
        ),
    )(counts, psi, pot, proj, ham_corr, delta)


def on_device(
    wavefunctions, potential, projectors, hamiltonian_correction, delta_s, projector_count
):
    bands, cx, ny, nz = wavefunctions.shape
    groups = lax.axis_size("band")
    doms = lax.axis_size("dom")
    lines = groups // 2
    mine = lax.axis_index("band")
    line, side = mine // 2, mine % 2
    volume = 1.0 / (cx * ny * nz * doms)
    atoms, slots = hamiltonian_correction.shape[:2]
    proj = projectors.reshape(atoms * slots, cx, ny, nz)
    fused = doms == QUADS and bands % 128 == 0
    grid = gram(
        wavefunctions, potential, proj, jnp.transpose(hamiltonian_correction, (1, 0, 2)),
        jnp.transpose(delta_s, (1, 0, 2)), projector_count, lines, doms, fused, volume,
    )
    if fused:
        return grid[0], grid[1]
    here = (jnp.arange(lines, dtype=jnp.int32) == line)[:, None, None, None]
    both = lax.psum(grid.reshape(lines, QUADS, bands, bands), "dom")
    lanes = [[at * 2 + s for at in range(lines)] for s in range(2)]
    mirrored = lax.all_to_all(both, "band", 0, 0, axis_index_groups=lanes, tiled=True)
    swapped = lax.ppermute(both, "band", [(i, i ^ 1) for i in range(groups)])
    crossed = (jnp.arange(QUADS, dtype=jnp.int32) >= 2)[None, :, None, None]
    total = volume * jnp.where(crossed, swapped, both) + volume * jnp.where(here, 0.0, jnp.swapaxes(mirrored, 2, 3))
    total = total.reshape(lines, 2, 2, bands, bands)
    by_side = jnp.where(side == 0, total, total[:, ::-1])
    final = jnp.transpose(by_side, (2, 3, 0, 1, 4)).reshape(2, bands, groups * bands)
    return final[0], final[1]


def solution(mesh):
    placed = (
        P("band", "dom", None, None),
        P("dom", None, None),
        P("dom", None, None, None, None),
        P("dom", None, None),
        P("dom", None, None),
        P("dom"),
    )
    return jax.shard_map(
        on_device,
        mesh=mesh,
        in_specs=placed,
        out_specs=(P("band", None), P("band", None)),
        check_vma=False,
    )
```

```python
import functools

import jax
import jax.numpy as jnp
from jax import lax
from jax.experimental import pallas as pl
from jax.experimental.pallas import tpu as pltpu
from jax.sharding import PartitionSpec as P

MESH = pl.DeviceIdType.MESH
CONTRACT_LAST = (((1,), (1,)), ((), ()))
MATMUL = (((1,), (0,)), ((), ()))
QUADS = 4
WINDOW = 4
SWAP_WINDOW = 4
HALO_AHEAD = 6


def parts(value):
    high = value.astype(jnp.bfloat16)
    low = (value - high.astype(jnp.float32)).astype(jnp.bfloat16)
    return high, low


def three(left, right, dims, axis):
    (left_high, left_low), (right_high, right_low) = left, right
    return lax.dot_general(
        jnp.concatenate([left_high, left_high, left_low], axis=1),
        jnp.concatenate([right_high, right_low, right_high], axis=axis),
        dims, preferred_element_type=jnp.float32,
    )


def exact(left, right):
    return lax.dot_general(
        left, right, MATMUL, precision=lax.Precision.HIGHEST, preferred_element_type=jnp.float32
    )


def remote(src, dst, send, recv, where):
    return pltpu.make_async_remote_copy(
        src_ref=src, dst_ref=dst, send_sem=send, recv_sem=recv,
        device_id=where, device_id_type=MESH,
    )


def gram_kernel(lines, doms, fused, volume, counts, psi_in, pot, proj_in, ham_corr, delta, *scratch):
    result, scratch = scratch[0], scratch[1:]
    (
        nat, packed, partner, halo, partner_halo, slots_r, slots_l, lhs_high, lhs_low,
        own_edge, full_edge, left_edge, edges_r, edges_l, proj, sym, coef, coef_below, coup_high, coup_low,
        load_sem, proj_sem, swap_send, swap_recv, halo_send, halo_recv, fwd_send, fwd_recv,
        right_send, right_recv, left_send, left_recv,
        right_edge_send, right_edge_recv, left_edge_send, left_edge_recv,
        coef_send, coef_recv, pair_send, pair_recv,
    ) = scratch[:40]
    rows, bands, nz = nat.shape
    cx, ny = pot.shape[:2]
    lane_half = nz // 2
    half = rows // 2
    per_y = cx // 2
    steps = ny // 2
    phases = lines - 2
    hops = lines - 1
    last = lines - 1
    window = min(WINDOW, ny)
    swap_window = min(SWAP_WINDOW, ny)
    halo_ahead = min(HALO_AHEAD, ny)
    slots, atoms = ham_corr.shape[:2]
    used = atoms * slots
    live = -(-used // 8) * 8
    width = sym.shape[1]
    grid = scratch[40] if fused else result

    mine = lax.axis_index("band")
    dom = lax.axis_index("dom")
    line = mine // 2
    side = mine % 2
    pair = line * 2 + (1 - side)
    upper = jnp.minimum(line + 1, last) * 2 + side
    lower = jnp.maximum(line - 1, 0) * 2 + side
    dom_next = (dom + 1) % doms
    dom_prev = (dom + doms - 1) % doms

    def loads(y):
        copies = []
        for p in range(cx):
            r = y * cx + p
            copies.append(pltpu.make_async_copy(psi_in.at[:, p, y], nat.at[r], load_sem.at[y]))
        return copies

    def proj_loads(y):
        copies = []
        for p in range(cx):
            r = y * cx + p
            copies.append(pltpu.make_async_copy(proj_in.at[:, p, y], proj.at[r], proj_sem.at[0]))
        return copies

    def start_loads(y, carry):
        for copy in loads(y):
            copy.start()
        return carry

    def start_proj(y, carry):
        for copy in proj_loads(y):
            copy.start()
        return carry

    if fused:
        combine = Combine(lines, volume, grid, result, line, side, pair, dom, scratch[41:])
    lax.fori_loop(0, ny, start_loads, 0)
    lax.fori_loop(0, ny, start_proj, 0)

    barrier = pltpu.get_barrier_semaphore()
    pl.semaphore_signal(barrier, inc=1, device_id={"band": pair}, device_id_type=MESH)

    @pl.when(line > 0)
    def _():
        pl.semaphore_signal(barrier, inc=1, device_id={"band": lower}, device_id_type=MESH)

    @pl.when(line < last)
    def _():
        pl.semaphore_signal(barrier, inc=1, device_id={"band": upper}, device_id_type=MESH)

    for ahead in range(1, doms):
        pl.semaphore_signal(barrier, inc=1, device_id={"dom": (dom + ahead) % doms}, device_id_type=MESH)
    pl.semaphore_wait(barrier, doms + jnp.minimum(line, 1) + jnp.minimum(last - line, 1))

    def swap(y):
        at = pl.ds(y * cx, cx)
        return remote(nat.at[at], partner.at[at], swap_send.at[y % swap_window], swap_recv.at[y], {"band": pair})

    def planes(src, dst, send, recv, y):
        return [
            remote(src.at[y * cx + p], dst.at[edge, y], send.at[0], recv.at[y], {"dom": to})
            for edge, p, to in ((0, cx - 1, dom_next), (1, 0, dom_prev))
        ]

    def both_planes(dst, send, recv, y):
        return remote(dst.at[:, y], dst.at[:, y], send.at[0], recv.at[y], {"dom": dom_next})

    def halos(y):
        return planes(nat, halo, halo_send, halo_recv, y)

    def forwards(y):
        return planes(partner, partner_halo, fwd_send, fwd_recv, y)

    class Way:
        def __init__(self, base, place, slots, edges, send, recv, edge_send, edge_recv, to):
            self.base, self.place, self.slots, self.edges = base, place, slots, edges
            self.send, self.recv, self.edge_send, self.edge_recv, self.to = send, recv, edge_send, edge_recv, to
            self.count = jnp.where(place == 0, 0, jnp.where(place == 1, 2, jnp.where(place == last, last - 1, place)))
            self.own_first = place < last - 1
            self.shift = jnp.where(self.own_first, 1, 0)
            self.items = jnp.where(place == 0, 2, place + 1) * ny

        def source(self, f):
            from_place = jnp.where(
                self.place == 1, 0, jnp.where(self.place == last, self.place - 2 - f, self.place - 1 - f)
            )
            from_place = jnp.clip(from_place, 0, last)
            return from_place if self.base == 0 else last - from_place

        def half_of(self, f):
            return jnp.where(self.place == 1, 1 - self.base, self.base) if f == 1 else self.base

        def gets(self, f):
            return self.count > f

        def passes(self, f):
            return (self.place >= 1) & (self.place < last) & (self.place > f)

        def own(self, y):
            at = pl.ds(y * per_y, per_y)
            return remote(
                packed.at[self.base, at], self.slots.at[0, at], self.send.at[y % window], self.recv.at[0, y],
                {"band": self.to},
            )

        def extra(self, y):
            at = pl.ds(y * per_y, per_y)
            return remote(
                packed.at[1 - self.base, at], self.slots.at[1, at], self.send.at[(ny + y) % window], self.recv.at[1, y],
                {"band": self.to},
            )

        def hop(self, f, y):
            at = pl.ds(y * per_y, per_y)
            q = jnp.minimum(f + self.shift, phases - 1)
            slot = jnp.where(self.own_first, (q * ny + y) % window, window)
            return remote(
                self.slots.at[f, at], self.slots.at[q, at], self.send.at[slot], self.recv.at[q, y], {"band": self.to}
            )

        def arrival(self, f, y):
            at = pl.ds(y * per_y, per_y)
            return remote(
                self.slots.at[f, at], self.slots.at[f, at], self.send.at[0], self.recv.at[f, y], {"band": self.to}
            )

        def start_item(self, item):
            q, y = item // ny, item % ny

            @pl.when(q == 0)
            def _():
                self.own(y).start()

            @pl.when((q == 1) & (self.place == 0))
            def _():
                self.extra(y).start()

            @pl.when((q >= 1) & (self.place >= 1))
            def _():
                self.hop(jnp.clip(q - 1, 0, phases - 1), y).start()

        def sent(self, item):
            q, y = item // ny, item % ny
            at = pl.ds(y * per_y, per_y)
            remote(
                packed.at[self.base, at], self.slots.at[q, at], self.send.at[item % window], self.recv.at[q, y],
                {"band": self.to},
            ).wait_send()

        def pace(self, item):
            @pl.when(self.own_first & (item < self.items))
            def _():
                self.sent(item - window)
                self.start_item(item)

        def own_edge(self):
            return remote(
                own_edge.at[self.base], self.edges.at[0], self.edge_send.at[0], self.edge_recv.at[0], {"band": self.to}
            )

        def extra_edge(self):
            return remote(
                own_edge.at[1 - self.base], self.edges.at[1], self.edge_send.at[1], self.edge_recv.at[1],
                {"band": self.to},
            )

        def edge_hop(self, f):
            q = jnp.minimum(f + self.shift, phases - 1)
            return remote(
                self.edges.at[f], self.edges.at[q], self.edge_send.at[q], self.edge_recv.at[q], {"band": self.to}
            )

        def edge_arrival(self, f):
            return remote(
                self.edges.at[f], self.edges.at[f], self.edge_send.at[f], self.edge_recv.at[f], {"band": self.to}
            )

    ways = (
        Way(0, line, slots_r, edges_r, right_send, right_recv, right_edge_send, right_edge_recv, upper),
        Way(1, last - line, slots_l, edges_l, left_send, left_recv, left_edge_send, left_edge_recv, lower),
    )
    live_rows = pl.ds(0, live)
    coef_swap = remote(
        coef.at[0, live_rows], coef.at[1, live_rows], pair_send.at[0], pair_recv.at[0], {"band": pair}
    )

    def coef_hop(dist):
        src = coef.at[0, live_rows] if dist == 1 else coef_below.at[dist - 2, live_rows]
        return remote(
            src, coef_below.at[dist - 1, live_rows], coef_send.at[dist - 1], coef_recv.at[dist - 1], {"band": upper}
        )

    lanes = lax.broadcasted_iota(jnp.int32, (bands, nz), 1)
    low_lanes = lanes < lane_half

    def pack(first, second):
        low = low_lanes[: first.shape[0]]
        return (
            jnp.where(low, first, pltpu.roll(second, lane_half, 1)),
            jnp.where(low, pltpu.roll(first, lane_half, 1), second),
        )

    def take(f, y):
        for way in ways:
            @pl.when(way.passes(f) & (way.shift == 0))
            def _(way=way):
                way.arrival(f, y).wait_recv()
                way.hop(f, y).start()

        for way in ways:
            way.pace(f * ny + y + window)

        for way in ways:
            @pl.when(way.gets(f) & ~(way.passes(f) & (way.shift == 0)))
            def _(way=way):
                way.arrival(f, y).wait_recv()

    def start_own(y):
        for way in ways:
            @pl.when(way.own_first)
            def _(way=way):
                way.own(y).start()

    left_edge[...] = jnp.zeros_like(left_edge)

    def begin(y, carry):
        at = pl.ds(y * cx, cx)
        pltpu.make_async_copy(nat.at[at], nat.at[at], load_sem.at[y]).wait()

        @pl.when(y < swap_window)
        def _():
            swap(y).start()

        @pl.when(y < halo_ahead)
        def _():
            for copy in halos(y):
                copy.start()

        for pp in range(per_y):
            k = y * per_y + pp
            first, second = pack(nat[2 * k], nat[2 * k + 1])
            packed[0, k] = first
            packed[1, k] = second

        @pl.when((y >= 1) & (y <= window))
        def _():
            start_own(y - 1)

        return carry

    lax.fori_loop(0, ny, begin, 0)
    if window == ny:
        start_own(ny - 1)

    def gather_edge(r, carry):
        here = nat[r]
        spot = (lanes == r) | (lanes == r + lane_half)
        return jnp.where(spot, pltpu.roll(here, (r + lane_half) % nz, 1), carry)

    edge = lax.fori_loop(0, rows, gather_edge, jnp.zeros((bands, nz), jnp.float32), unroll=8)
    full_edge[...] = edge
    for h, value in enumerate(pack(edge[: bands // 2], edge[bands // 2 :])):
        own_edge[h] = value

    take(0, 0)
    for kind, source in enumerate((ham_corr, delta)):
        total = jnp.zeros((width, width), jnp.float32)
        for a in range(atoms):
            wide = lax.broadcasted_iota(jnp.int32, (slots, width), 0) + a * slots
            place = wide == lax.broadcasted_iota(jnp.int32, (slots, width), 1)
            place = place & (wide - a * slots < counts[a])
            tall = lax.broadcasted_iota(jnp.int32, (width, slots), 1) + a * slots
            tall_place = tall == lax.broadcasted_iota(jnp.int32, (width, slots), 0)
            tall_place = tall_place & (tall - a * slots < counts[a])
            total = total + exact(tall_place.astype(jnp.float32), exact(source[:, a], place.astype(jnp.float32)))
        sym[kind] = (0.5 / volume) * (total + jnp.transpose(total))

    coef[0] = jnp.zeros((width, bands), jnp.float32)
    if live < width:
        unused = jnp.zeros((width - live, bands), jnp.float32)
        coef[1, pl.ds(live, width - live)] = unused
        for slot in range(hops):
            coef_below[slot, pl.ds(live, width - live)] = unused

    def coef_body(y, carry):
        left, right = [], []
        for p in range(cx):
            r = y * cx + p
            proj_high, proj_low = parts(proj[r])
            high, low = parts(nat[r])
            left += [proj_high, proj_high, proj_low]
            right += [high, low, high]
        coef[0, pl.ds(0, used)] += lax.dot_general(
            jnp.concatenate(left, axis=1), jnp.concatenate(right, axis=1), CONTRACT_LAST,
            preferred_element_type=jnp.float32,
        )
        return carry

    pltpu.make_async_copy(proj, proj, proj_sem.at[0]).wait()
    lax.fori_loop(0, ny // 2, coef_body, 0)
    take(0, 1)
    lax.fori_loop(ny // 2, ny, coef_body, 0)
    take(0, 2)

    for way in ways:
        @pl.when(way.own_first)
        def _(way=way):
            way.own_edge().start()

        @pl.when(way.place == 0)
        def _(way=way):
            way.extra_edge().start()

    coef_swap.start()

    @pl.when(line < last)
    def _():
        coef_hop(1).start()

    grid[...] = jnp.zeros_like(grid)

    def operand(src, edges, group, y):
        up = (y + ny - 1) % ny
        down = (y + 1) % ny
        edge = left_edge[group]
        for pp in range(per_y):
            k = y * per_y + pp
            hpsi, own = [], []
            for t in range(2):
                p = 2 * pp + t
                r = y * cx + p
                here = src[r]
                before = edges[0, y] if p == 0 else src[r - 1]
                after = edges[1, y] if p == cx - 1 else src[r + 1]
                beside = before + after
                beside = beside + src[up * cx + p]
                beside = beside + src[down * cx + p]
                beside = beside + jnp.where(lanes % lane_half == 0, 0.0, pltpu.roll(here, 1, 1))
                beside = beside + pltpu.roll(here, nz - 1, 1)
                hpsi.append(0.5 * (6.0 * here - beside) + pot[p, pl.ds(y, 1)] * here)
                own.append(here)
                spot = (lanes == r) | (lanes == r + lane_half)
                edge = jnp.where(spot, -0.5 * pltpu.roll(here, (r + lane_half + 1) % nz, 1), edge)
            for slot, both in ((2 * group, pack(*hpsi)), (2 * group + 1, pack(*own))):
                for h in range(2):
                    high, low = parts(both[h])
                    lhs_high[h * half + k, pl.ds(slot * bands, bands)] = high
                    lhs_low[h * half + k, pl.ds(slot * bands, bands)] = low
        left_edge[group] = edge

    def accumulate(group, source, row, right_row, count):
        where = pl.ds(group * 2 * bands, 2 * bands)
        left, right = [], []
        for i in range(count):
            high, low = lhs_high[row + i, where], lhs_low[row + i, where]
            other_high, other_low = right_row(i)
            left += [high, high, low]
            right += [other_high, other_low, other_high]
        grid[source, where] += lax.dot_general(
            jnp.concatenate(left, axis=1), jnp.concatenate(right, axis=1), CONTRACT_LAST,
            preferred_element_type=jnp.float32,
        )

    def with_own(group, y, ys):
        own = pl.ds(bands, bands)
        for h in range(2):
            row = h * half + y * per_y
            accumulate(
                group, line, row, lambda i, row=row: (lhs_high[row + i, own], lhs_low[row + i, own]), ys * per_y
            )

    def with_moved(group, way, f, y, ys):
        accumulate(
            group, way.source(f), way.half_of(f) * half + y * per_y,
            lambda i: parts(way.slots[f, y * per_y + i]), ys * per_y,
        )

    def moved_all(group, f, y, ys):
        for way in ways:
            @pl.when(way.gets(f))
            def _(way=way):
                with_moved(group, way, f, y, ys)

    def partner_operand(y):
        both_planes(partner_halo, fwd_send, fwd_recv, y).wait_recv()
        operand(partner, partner_halo, 1, y)

    def with_edges(group):
        into = pl.ds(2 * group * bands, bands)
        low = low_lanes[: bands // 2]
        right = [full_edge[...]]
        found = []
        for way in ways:
            for f in range(phases):
                here = way.edges[f]
                turned = pltpu.roll(here, lane_half, 1)
                first = way.half_of(f) == 0
                keep = (low ^ (way.half_of(f) == 1)) & way.gets(f)
                right.append(jnp.where(keep, jnp.where(first, here, turned), 0.0))
                right.append(jnp.where(keep, jnp.where(first, turned, here), 0.0))
                found.append((way, f))
        added = three(parts(left_edge[group]), parts(jnp.concatenate(right, axis=0)), CONTRACT_LAST, 1)
        grid[line, into] += added[:, :bands]
        for at, (way, f) in enumerate(found):
            @pl.when(way.gets(f))
            def _(way=way, f=f, at=at):
                grid[way.source(f), into] += added[:, (at + 1) * bands : (at + 2) * bands]

    def edge_stage(f):
        for way in ways:
            @pl.when(way.gets(f))
            def _(way=way):
                way.edge_arrival(f).wait_recv()

            @pl.when(way.passes(f))
            def _(way=way):
                way.edge_hop(f).start()

    def couple(group):
        for kind in range(2):
            coupled = jnp.transpose(exact(sym[kind], coef[group]))
            high, low = parts(coupled)
            where = pl.ds((2 * group + kind) * bands, bands)
            coup_high[where] = high
            coup_low[where] = low

    def project(source, right):
        grid[source] += three((coup_high[...], coup_low[...]), parts(right), MATMUL, 0)

    def coef_stage(dist):
        @pl.when(line >= dist)
        def _():
            coef_hop(dist).wait_recv()

        if dist < hops:
            @pl.when((line >= dist) & (line < last))
            def _():
                coef_hop(dist + 1).start()

        @pl.when(line >= dist)
        def _():
            project(line - dist, coef_below[dist - 1])

    def partner_row(u, carry):
        swap(u).wait_recv()
        for copy in forwards(u):
            copy.start()

        @pl.when(u + swap_window < ny)
        def _():
            swap(u).wait_send()
            swap(u + swap_window).start()

        @pl.when(u >= 2)
        def _():
            partner_operand(u - 1)
            with_own(1, u - 1, 1)
            moved_all(1, 0, u - 1, 1)

        return carry

    def first_phase(t, carry):
        for y in (halo_ahead + 2 * t, halo_ahead + 2 * t + 1):
            @pl.when(y < ny)
            def _(y=y):
                for copy in halos(y):
                    copy.start()

        @pl.when(t >= 2)
        def _():
            take(0, 2 * t)

        for y in (2 * t, 2 * t + 1):
            both_planes(halo, halo_send, halo_recv, y).wait_recv()
            operand(nat, halo, 0, y)
        with_own(0, 2 * t, 2)

        @pl.when(t >= 2)
        def _():
            take(0, 2 * t + 1)

        @pl.when(t == 0)
        def _():
            take(0, 3)

        moved_all(0, 0, 2 * t, 2)
        partner_row(t, 0)
        return carry

    lax.fori_loop(0, steps, first_phase, 0)

    coef_swap.wait_recv()
    couple(0)
    couple(1)
    project(line, coef[0])
    edge_stage(0)
    coef_stage(1)

    def second_phase(t, carry):
        take(1, 2 * t)
        partner_row(steps + t, 0)
        take(1, 2 * t + 1)
        moved_all(0, 1, 2 * t, 2)
        for y in (2 * t, 2 * t + 1):
            @pl.when(y != 0)
            def _(y=y):
                moved_all(1, 1, y, 1)

        for stage in range(1, hops):
            @pl.when(t == min(2 * stage + 1, steps - 3))
            def _(stage=stage):
                if stage < phases:
                    edge_stage(stage)
                coef_stage(stage + 1)

        @pl.when(t == steps - 3)
        def _():
            with_edges(0)

        return carry

    lax.fori_loop(0, steps - 1, second_phase, 0)
    between = (line > 0) & (line < last)
    take(1, ny - 2)
    partner_row(ny - 1, 0)

    @pl.when(between)
    def _():
        take(1, ny - 1)

    partner_operand(0)
    with_own(1, 0, 1)
    moved_all(1, 0, 0, 1)
    moved_all(1, 1, 0, 1)

    @pl.when(~between)
    def _():
        take(1, ny - 1)

    moved_all(0, 1, ny - 2, 2)
    early = fused and phases == 2
    if early:
        combine.send(0)
    partner_operand(ny - 1)
    with_own(1, ny - 1, 1)
    moved_all(1, 0, ny - 1, 1)
    if early:
        combine.reduce(0)
    moved_all(1, 1, ny - 2, 2)
    with_edges(1)
    for f in range(2, phases):
        def later_phase(t, carry, f=f):
            take(f, 2 * t)
            take(f, 2 * t + 1)
            moved_all(0, f, 2 * t, 2)
            moved_all(1, f, 2 * t, 2)
            return carry

        lax.fori_loop(0, steps, later_phase, 0)

    if fused:
        if not early:
            combine.send(0)
            combine.reduce(0)
        combine.send(1)
        combine.reduce(1)
        combine.rest()

    for y in range(ny - swap_window, ny):
        swap(y).wait_send()
    remote(halo, halo, halo_send.at[0], halo_recv.at[0], {"dom": dom_next}).wait_send()
    remote(partner_halo, partner_halo, fwd_send.at[0], fwd_recv.at[0], {"dom": dom_next}).wait_send()
    for way in ways:
        @pl.when(way.own_first)
        def _(way=way):
            for ahead in range(window):
                way.sent(way.items - window + ahead)

        @pl.when(way.place == last - 1)
        def _(way=way):
            remote(
                way.slots, way.slots, way.send.at[window], way.recv.at[0, 0], {"band": way.to}
            ).wait_send()

    coef_swap.wait_send()
    for dist in range(1, lines):
        @pl.when((line >= dist - 1) & (line < last))
        def _(dist=dist):
            coef_hop(dist).wait_send()
    for way in ways:
        @pl.when(way.own_first)
        def _(way=way):
            way.own_edge().wait_send()

        @pl.when(way.place == 0)
        def _(way=way):
            way.extra_edge().wait_send()

        for f in range(phases):
            @pl.when(way.passes(f))
            def _(way=way, f=f):
                way.edge_hop(f).wait_send()


class Combine:
    def __init__(self, lines, volume, grid, out, line, side, pair, dom, scratch):
        (
            from_core, both, from_chip, total, mirror, swapped,
            core_send, core_recv, chip_send, chip_recv, line_send, line_recv, side_send, side_recv,
            near_send, near_recv, far_send, far_recv, pass_send, pass_recv, result, out_sem,
        ) = scratch
        bands = grid.shape[2]
        core = dom % 2
        kind = dom // 2
        other_core = kind * 2 + (1 - core)
        other_chip = (1 - kind) * 2 + core
        my_kind = pl.ds(pl.multiple_of(kind * bands, bands), bands)
        their_kind = pl.ds(pl.multiple_of((1 - kind) * bands, bands), bands)
        turn = jnp.where(line == 0, 1, 0)
        others = [(line + 1 + (k + turn) % (lines - 1)) % lines for k in range(lines - 1)]
        order = others + [line]
        closing = [line] + others

        def rows(group):
            return pl.ds(group * 2 * bands, 2 * bands)

        def to_core(group, s):
            return remote(
                grid.at[s, rows(group)], from_core.at[s], core_send.at[0], core_recv.at[s], {"dom": other_core}
            )

        def to_chip(s):
            return remote(both.at[s, their_kind], from_chip.at[s], chip_send.at[0], chip_recv.at[s], {"dom": other_chip})

        def to_line(s):
            return remote(
                total.at[s], mirror.at[line], line_send.at[0], line_recv.at[line], {"band": s * 2 + side}
            )

        def from_line(s):
            return remote(
                total.at[s], mirror.at[s], line_send.at[0], line_recv.at[s], {"band": s * 2 + side}
            )

        def to_side(s):
            return remote(total.at[s], swapped.at[s], side_send.at[0], side_recv.at[s], {"band": pair})

        def piece(s, group, k, send, recv, to):
            block = s * 2 + (side if group == 0 else 1 - side)
            at = result.at[k, :, pl.ds(pl.multiple_of(block * bands, bands), bands)]
            return remote(at, at, send.at[0], recv.at[s], {"dom": to})

        def near(s, group):
            return piece(s, group, kind, near_send, near_recv, other_core)

        def far(s, group, k):
            return piece(s, group, k, far_send, far_recv, other_chip)

        def onward(s, group):
            return piece(s, group, 1 - kind, pass_send, pass_recv, other_core)

        def send(group):
            @pl.when(core == 1 - group)
            def _():
                for s in order:
                    to_core(group, s).start()

        def flush(s, group, k):
            block = s * 2 + (side if group == 0 else 1 - side)
            at = (k, slice(None), pl.ds(pl.multiple_of(block * bands, bands), bands))
            pltpu.make_async_copy(result.at[at], out.at[at], out_sem.at[0]).start()

        def reduce(group):
            @pl.when(core == group)
            def _():
                for s in order:
                    to_core(group, s).wait_recv()
                    both[s] = grid[s, rows(group)] + from_core[s]
                    to_chip(s).start()

        def work(group):
            for s in order:
                to_chip(s).wait_recv()
                total[s] = both[s, my_kind] + from_chip[s]
                if s is not line:
                    to_line(s).start()
                if group:
                    to_side(s).start()
            for s in closing:
                if group:
                    to_side(s).wait_recv()
                    value = swapped[s]
                else:
                    value = total[s]
                if s is not line:
                    from_line(s).wait_recv()
                    value = value + jnp.transpose(mirror[s])
                block = s * 2 + (side if group == 0 else 1 - side)
                result[kind, :, pl.ds(pl.multiple_of(block * bands, bands), bands)] = volume * value
                far(s, group, kind).start()
                near(s, group).start()
                flush(s, group, kind)
            for s in closing:
                near(s, 1 - group).wait_recv()
                flush(s, 1 - group, kind)
            for s in closing:
                far(s, group, 1 - kind).wait_recv()
                onward(s, group).start()
                flush(s, group, 1 - kind)
            for s in closing:
                onward(s, 1 - group).wait_recv()
                flush(s, 1 - group, 1 - kind)
            pltpu.make_async_copy(result, result, out_sem.at[0]).wait()
            for held, send, recv in (
                (from_core, core_send, core_recv), (from_chip, chip_send, chip_recv),
                (mirror.at[pl.ds(0, lines - 1)], line_send, line_recv), (total, near_send, near_recv),
                (total, far_send, far_recv), (total, pass_send, pass_recv),
            ):
                remote(held, held, send.at[0], recv.at[0], {"dom": other_core}).wait_send()
            if group:
                remote(swapped, swapped, side_send.at[0], side_recv.at[0], {"dom": other_core}).wait_send()

        def rest():
            for group in range(2):
                @pl.when(core == group)
                def _(group=group):
                    work(group)

        self.send = send
        self.reduce = reduce
        self.rest = rest


def gram(psi, pot, proj, ham_corr, delta, counts, lines, doms, fused, volume):
    bands, cx, ny, nz = psi.shape
    rows = cx * ny
    half = rows // 2
    used = proj.shape[0]
    width = -(-used // 128) * 128
    hops = lines - 1
    phases = lines - 2
    window = min(WINDOW, ny) + 1
    f32 = jnp.float32
    dma = pltpu.SemaphoreType.DMA
    vmem = pl.BlockSpec(memory_space=pltpu.VMEM)
    hbm = pl.BlockSpec(memory_space=pl.ANY)
    scratch = [
        pltpu.VMEM((rows, bands, nz), f32),
        pltpu.VMEM((2, half, bands, nz), f32),
        pltpu.VMEM((rows, bands, nz), f32),
        pltpu.VMEM((2, ny, bands, nz), f32),
        pltpu.VMEM((2, ny, bands, nz), f32),
        pltpu.VMEM((phases, half, bands, nz), f32),
        pltpu.VMEM((phases, half, bands, nz), f32),
        pltpu.VMEM((rows, QUADS * bands, nz), jnp.bfloat16),
        pltpu.VMEM((rows, QUADS * bands, nz), jnp.bfloat16),
        pltpu.VMEM((2, bands // 2, nz), f32),
        pltpu.VMEM((bands, nz), f32),
        pltpu.VMEM((2, bands, nz), f32),
        pltpu.VMEM((phases, bands // 2, nz), f32),
        pltpu.VMEM((phases, bands // 2, nz), f32),
        pltpu.VMEM((rows, used, nz), f32),
        pltpu.VMEM((2, width, width), f32),
        pltpu.VMEM((2, width, bands), f32),
        pltpu.VMEM((hops, width, bands), f32),
        pltpu.VMEM((QUADS * bands, width), jnp.bfloat16),
        pltpu.VMEM((QUADS * bands, width), jnp.bfloat16),
        dma((ny,)), dma((1,)), dma((min(SWAP_WINDOW, ny),)), dma((ny,)), dma((1,)), dma((ny,)), dma((1,)), dma((ny,)),
        dma((window,)), dma((phases, ny)), dma((window,)), dma((phases, ny)),
        dma((phases,)), dma((phases,)), dma((phases,)), dma((phases,)),
        dma((hops,)), dma((hops,)), dma((1,)), dma((1,)),
    ]
    if fused:
        columns = 2 * lines * bands
        shape = jax.ShapeDtypeStruct((2, bands, columns), f32)
        placed = hbm
        scratch += [
            pltpu.VMEM((lines, QUADS * bands, bands), f32),
            pltpu.VMEM((lines, 2 * bands, bands), f32),
            pltpu.VMEM((lines, 2 * bands, bands), f32),
            pltpu.VMEM((lines, bands, bands), f32),
            pltpu.VMEM((lines, bands, bands), f32),
            pltpu.VMEM((lines, bands, bands), f32),
            pltpu.VMEM((lines, bands, bands), f32),
        ] + [dma((1,)), dma((lines,))] * 7 + [pltpu.VMEM((2, bands, columns), f32), dma((1,))]
    else:
        shape = jax.ShapeDtypeStruct((lines, QUADS * bands, bands), f32)
        placed = vmem
    return pl.pallas_call(
        functools.partial(gram_kernel, lines, doms, fused, volume),
        out_shape=shape,
        in_specs=[pl.BlockSpec(memory_space=pltpu.SMEM), hbm, vmem, hbm, vmem, vmem],
        out_specs=placed,
        scratch_shapes=scratch,
        compiler_params=pltpu.CompilerParams(
            collective_id=0, has_side_effects=True, vmem_limit_bytes=62 * 1024 * 1024
        ),
    )(counts, psi, pot, proj, ham_corr, delta)


def on_device(
    wavefunctions, potential, projectors, hamiltonian_correction, delta_s, projector_count
):
    bands, cx, ny, nz = wavefunctions.shape
    groups = lax.axis_size("band")
    doms = lax.axis_size("dom")
    lines = groups // 2
    mine = lax.axis_index("band")
    line, side = mine // 2, mine % 2
    volume = 1.0 / (cx * ny * nz * doms)
    atoms, slots = hamiltonian_correction.shape[:2]
    proj = projectors.reshape(atoms * slots, cx, ny, nz)
    fused = doms == QUADS and bands % 128 == 0
    grid = gram(
        wavefunctions, potential, proj, jnp.transpose(hamiltonian_correction, (1, 0, 2)),
        jnp.transpose(delta_s, (1, 0, 2)), projector_count, lines, doms, fused, volume,
    )
    if fused:
        return grid[0], grid[1]
    here = (jnp.arange(lines, dtype=jnp.int32) == line)[:, None, None, None]
    both = lax.psum(grid.reshape(lines, QUADS, bands, bands), "dom")
    lanes = [[at * 2 + s for at in range(lines)] for s in range(2)]
    mirrored = lax.all_to_all(both, "band", 0, 0, axis_index_groups=lanes, tiled=True)
    swapped = lax.ppermute(both, "band", [(i, i ^ 1) for i in range(groups)])
    crossed = (jnp.arange(QUADS, dtype=jnp.int32) >= 2)[None, :, None, None]
    total = volume * jnp.where(crossed, swapped, both) + volume * jnp.where(here, 0.0, jnp.swapaxes(mirrored, 2, 3))
    total = total.reshape(lines, 2, 2, bands, bands)
    by_side = jnp.where(side == 0, total, total[:, ::-1])
    final = jnp.transpose(by_side, (2, 3, 0, 1, 4)).reshape(2, bands, groups * bands)
    return final[0], final[1]


def solution(mesh):
    placed = (
        P("band", "dom", None, None),
        P("dom", None, None),
        P("dom", None, None, None, None),
        P("dom", None, None),
        P("dom", None, None),
        P("dom"),
    )
    return jax.shard_map(
        on_device,
        mesh=mesh,
        in_specs=placed,
        out_specs=(P("band", None), P("band", None)),
        check_vma=False,
    )
```

```python
import functools

import jax
import jax.numpy as jnp
from jax import lax
from jax.experimental import pallas as pl
from jax.experimental.pallas import tpu as pltpu
from jax.sharding import PartitionSpec as P

MESH = pl.DeviceIdType.MESH
CONTRACT_LAST = (((1,), (1,)), ((), ()))
MATMUL = (((1,), (0,)), ((), ()))
QUADS = 4
WINDOW = 4
SWAP_WINDOW = 4
HALO_AHEAD = 6


def parts(value):
    high = value.astype(jnp.bfloat16)
    low = (value - high.astype(jnp.float32)).astype(jnp.bfloat16)
    return high, low


def three(left, right, dims, axis):
    (left_high, left_low), (right_high, right_low) = left, right
    return lax.dot_general(
        jnp.concatenate([left_high, left_high, left_low], axis=1),
        jnp.concatenate([right_high, right_low, right_high], axis=axis),
        dims, preferred_element_type=jnp.float32,
    )


def exact(left, right):
    return lax.dot_general(
        left, right, MATMUL, precision=lax.Precision.HIGHEST, preferred_element_type=jnp.float32
    )


def remote(src, dst, send, recv, where):
    return pltpu.make_async_remote_copy(
        src_ref=src, dst_ref=dst, send_sem=send, recv_sem=recv,
        device_id=where, device_id_type=MESH,
    )


def gram_kernel(lines, doms, fused, volume, counts, psi_in, pot, proj_in, ham_corr, delta, *scratch):
    result, scratch = scratch[0], scratch[1:]
    (
        nat, packed, partner, halo, partner_halo, slots_r, slots_l, lhs_high, lhs_low,
        own_edge, full_edge, left_edge, edges_r, edges_l, proj, sym, coef, coef_below, coup_high, coup_low,
        load_sem, proj_sem, swap_send, swap_recv, halo_send, halo_recv, fwd_send, fwd_recv,
        right_send, right_recv, left_send, left_recv,
        right_edge_send, right_edge_recv, left_edge_send, left_edge_recv,
        coef_send, coef_recv, pair_send, pair_recv,
    ) = scratch[:40]
    rows, bands, nz = nat.shape
    cx, ny = pot.shape[:2]
    lane_half = nz // 2
    half = rows // 2
    per_y = cx // 2
    steps = ny // 2
    phases = lines - 2
    hops = lines - 1
    last = lines - 1
    window = min(WINDOW, ny)
    swap_window = min(SWAP_WINDOW, ny)
    halo_ahead = min(HALO_AHEAD, ny)
    slots, atoms = ham_corr.shape[:2]
    used = atoms * slots
    live = -(-used // 8) * 8
    width = sym.shape[1]
    grid = scratch[40] if fused else result

    mine = lax.axis_index("band")
    dom = lax.axis_index("dom")
    line = mine // 2
    side = mine % 2
    pair = line * 2 + (1 - side)
    upper = jnp.minimum(line + 1, last) * 2 + side
    lower = jnp.maximum(line - 1, 0) * 2 + side
    dom_next = (dom + 1) % doms
    dom_prev = (dom + doms - 1) % doms

    def loads(y):
        copies = []
        for p in range(cx):
            r = y * cx + p
            copies.append(pltpu.make_async_copy(psi_in.at[:, p, y], nat.at[r], load_sem.at[y]))
        return copies

    def proj_loads(y):
        copies = []
        for p in range(cx):
            r = y * cx + p
            copies.append(pltpu.make_async_copy(proj_in.at[:, p, y], proj.at[r], proj_sem.at[0]))
        return copies

    def start_loads(y, carry):
        for copy in loads(y):
            copy.start()
        return carry

    def start_proj(y, carry):
        for copy in proj_loads(y):
            copy.start()
        return carry

    if fused:
        combine = Combine(lines, volume, grid, result, line, side, pair, dom, scratch[41:])
    lax.fori_loop(0, ny, start_loads, 0)
    lax.fori_loop(0, ny, start_proj, 0)

    barrier = pltpu.get_barrier_semaphore()
    pl.semaphore_signal(barrier, inc=1, device_id={"band": pair}, device_id_type=MESH)

    @pl.when(line > 0)
    def _():
        pl.semaphore_signal(barrier, inc=1, device_id={"band": lower}, device_id_type=MESH)

    @pl.when(line < last)
    def _():
        pl.semaphore_signal(barrier, inc=1, device_id={"band": upper}, device_id_type=MESH)

    for ahead in range(1, doms):
        pl.semaphore_signal(barrier, inc=1, device_id={"dom": (dom + ahead) % doms}, device_id_type=MESH)
    pl.semaphore_wait(barrier, doms + jnp.minimum(line, 1) + jnp.minimum(last - line, 1))

    def swap(y):
        at = pl.ds(y * cx, cx)
        return remote(nat.at[at], partner.at[at], swap_send.at[y % swap_window], swap_recv.at[y], {"band": pair})

    def planes(src, dst, send, recv, y):
        return [
            remote(src.at[y * cx + p], dst.at[edge, y], send.at[0], recv.at[y], {"dom": to})
            for edge, p, to in ((0, cx - 1, dom_next), (1, 0, dom_prev))
        ]

    def both_planes(dst, send, recv, y):
        return remote(dst.at[:, y], dst.at[:, y], send.at[0], recv.at[y], {"dom": dom_next})

    def halos(y):
        return planes(nat, halo, halo_send, halo_recv, y)

    def forwards(y):
        return planes(partner, partner_halo, fwd_send, fwd_recv, y)

    class Way:
        def __init__(self, base, place, slots, edges, send, recv, edge_send, edge_recv, to):
            self.base, self.place, self.slots, self.edges = base, place, slots, edges
            self.send, self.recv, self.edge_send, self.edge_recv, self.to = send, recv, edge_send, edge_recv, to
            self.count = jnp.where(place == 0, 0, jnp.where(place == 1, 2, jnp.where(place == last, last - 1, place)))
            self.own_first = place < last - 1
            self.shift = jnp.where(self.own_first, 1, 0)
            self.items = jnp.where(place == 0, 2, place + 1) * ny

        def source(self, f):
            from_place = jnp.where(
                self.place == 1, 0, jnp.where(self.place == last, self.place - 2 - f, self.place - 1 - f)
            )
            from_place = jnp.clip(from_place, 0, last)
            return from_place if self.base == 0 else last - from_place

        def half_of(self, f):
            return jnp.where(self.place == 1, 1 - self.base, self.base) if f == 1 else self.base

        def gets(self, f):
            return self.count > f

        def passes(self, f):
            return (self.place >= 1) & (self.place < last) & (self.place > f)

        def own(self, y):
            at = pl.ds(y * per_y, per_y)
            return remote(
                packed.at[self.base, at], self.slots.at[0, at], self.send.at[y % window], self.recv.at[0, y],
                {"band": self.to},
            )

        def extra(self, y):
            at = pl.ds(y * per_y, per_y)
            return remote(
                packed.at[1 - self.base, at], self.slots.at[1, at], self.send.at[(ny + y) % window], self.recv.at[1, y],
                {"band": self.to},
            )

        def hop(self, f, y):
            at = pl.ds(y * per_y, per_y)
            q = jnp.minimum(f + self.shift, phases - 1)
            slot = jnp.where(self.own_first, (q * ny + y) % window, window)
            return remote(
                self.slots.at[f, at], self.slots.at[q, at], self.send.at[slot], self.recv.at[q, y], {"band": self.to}
            )

        def arrival(self, f, y):
            at = pl.ds(y * per_y, per_y)
            return remote(
                self.slots.at[f, at], self.slots.at[f, at], self.send.at[0], self.recv.at[f, y], {"band": self.to}
            )

        def start_item(self, item):
            q, y = item // ny, item % ny

            @pl.when(q == 0)
            def _():
                self.own(y).start()

            @pl.when((q == 1) & (self.place == 0))
            def _():
                self.extra(y).start()

            @pl.when((q >= 1) & (self.place >= 1))
            def _():
                self.hop(jnp.clip(q - 1, 0, phases - 1), y).start()

        def sent(self, item):
            q, y = item // ny, item % ny
            at = pl.ds(y * per_y, per_y)
            remote(
                packed.at[self.base, at], self.slots.at[q, at], self.send.at[item % window], self.recv.at[q, y],
                {"band": self.to},
            ).wait_send()

        def pace(self, item):
            @pl.when(self.own_first & (item < self.items))
            def _():
                self.sent(item - window)
                self.start_item(item)

        def own_edge(self):
            return remote(
                own_edge.at[self.base], self.edges.at[0], self.edge_send.at[0], self.edge_recv.at[0], {"band": self.to}
            )

        def extra_edge(self):
            return remote(
                own_edge.at[1 - self.base], self.edges.at[1], self.edge_send.at[1], self.edge_recv.at[1],
                {"band": self.to},
            )

        def edge_hop(self, f):
            q = jnp.minimum(f + self.shift, phases - 1)
            return remote(
                self.edges.at[f], self.edges.at[q], self.edge_send.at[q], self.edge_recv.at[q], {"band": self.to}
            )

        def edge_arrival(self, f):
            return remote(
                self.edges.at[f], self.edges.at[f], self.edge_send.at[f], self.edge_recv.at[f], {"band": self.to}
            )

    ways = (
        Way(0, line, slots_r, edges_r, right_send, right_recv, right_edge_send, right_edge_recv, upper),
        Way(1, last - line, slots_l, edges_l, left_send, left_recv, left_edge_send, left_edge_recv, lower),
    )
    live_rows = pl.ds(0, live)
    coef_swap = remote(
        coef.at[0, live_rows], coef.at[1, live_rows], pair_send.at[0], pair_recv.at[0], {"band": pair}
    )

    def coef_hop(dist):
        src = coef.at[0, live_rows] if dist == 1 else coef_below.at[dist - 2, live_rows]
        return remote(
            src, coef_below.at[dist - 1, live_rows], coef_send.at[dist - 1], coef_recv.at[dist - 1], {"band": upper}
        )

    lanes = lax.broadcasted_iota(jnp.int32, (bands, nz), 1)
    low_lanes = lanes < lane_half

    def pack(first, second):
        low = low_lanes[: first.shape[0]]
        return (
            jnp.where(low, first, pltpu.roll(second, lane_half, 1)),
            jnp.where(low, pltpu.roll(first, lane_half, 1), second),
        )

    def take(f, y):
        for way in ways:
            @pl.when(way.passes(f) & (way.shift == 0))
            def _(way=way):
                way.arrival(f, y).wait_recv()
                way.hop(f, y).start()

        for way in ways:
            way.pace(f * ny + y + window)

        for way in ways:
            @pl.when(way.gets(f) & ~(way.passes(f) & (way.shift == 0)))
            def _(way=way):
                way.arrival(f, y).wait_recv()

    def start_own(y):
        for way in ways:
            @pl.when(way.own_first)
            def _(way=way):
                way.own(y).start()

    left_edge[...] = jnp.zeros_like(left_edge)

    def begin(y, carry):
        at = pl.ds(y * cx, cx)
        pltpu.make_async_copy(nat.at[at], nat.at[at], load_sem.at[y]).wait()

        @pl.when(y < swap_window)
        def _():
            swap(y).start()

        @pl.when(y < halo_ahead)
        def _():
            for copy in halos(y):
                copy.start()

        for pp in range(per_y):
            k = y * per_y + pp
            first, second = pack(nat[2 * k], nat[2 * k + 1])
            packed[0, k] = first
            packed[1, k] = second

        @pl.when((y >= 1) & (y <= window))
        def _():
            start_own(y - 1)

        return carry

    lax.fori_loop(0, ny, begin, 0)
    if window == ny:
        start_own(ny - 1)

    def gather_edge(r, carry):
        here = nat[r]
        spot = (lanes == r) | (lanes == r + lane_half)
        return jnp.where(spot, pltpu.roll(here, (r + lane_half) % nz, 1), carry)

    edge = lax.fori_loop(0, rows, gather_edge, jnp.zeros((bands, nz), jnp.float32), unroll=8)
    full_edge[...] = edge
    for h, value in enumerate(pack(edge[: bands // 2], edge[bands // 2 :])):
        own_edge[h] = value

    take(0, 0)
    for kind, source in enumerate((ham_corr, delta)):
        total = jnp.zeros((width, width), jnp.float32)
        for a in range(atoms):
            wide = lax.broadcasted_iota(jnp.int32, (slots, width), 0) + a * slots
            place = wide == lax.broadcasted_iota(jnp.int32, (slots, width), 1)
            place = place & (wide - a * slots < counts[a])
            tall = lax.broadcasted_iota(jnp.int32, (width, slots), 1) + a * slots
            tall_place = tall == lax.broadcasted_iota(jnp.int32, (width, slots), 0)
            tall_place = tall_place & (tall - a * slots < counts[a])
            total = total + exact(tall_place.astype(jnp.float32), exact(source[:, a], place.astype(jnp.float32)))
        sym[kind] = (0.5 / volume) * (total + jnp.transpose(total))

    coef[0] = jnp.zeros((width, bands), jnp.float32)
    if live < width:
        unused = jnp.zeros((width - live, bands), jnp.float32)
        coef[1, pl.ds(live, width - live)] = unused
        for slot in range(hops):
            coef_below[slot, pl.ds(live, width - live)] = unused

    def coef_body(y, carry):
        left, right = [], []
        for p in range(cx):
            r = y * cx + p
            proj_high, proj_low = parts(proj[r])
            high, low = parts(nat[r])
            left += [proj_high, proj_high, proj_low]
            right += [high, low, high]
        coef[0, pl.ds(0, used)] += lax.dot_general(
            jnp.concatenate(left, axis=1), jnp.concatenate(right, axis=1), CONTRACT_LAST,
            preferred_element_type=jnp.float32,
        )
        return carry

    pltpu.make_async_copy(proj, proj, proj_sem.at[0]).wait()
    lax.fori_loop(0, ny // 2, coef_body, 0)
    take(0, 1)
    lax.fori_loop(ny // 2, ny, coef_body, 0)
    take(0, 2)

    for way in ways:
        @pl.when(way.own_first)
        def _(way=way):
            way.own_edge().start()

        @pl.when(way.place == 0)
        def _(way=way):
            way.extra_edge().start()

    coef_swap.start()

    @pl.when(line < last)
    def _():
        coef_hop(1).start()

    grid[...] = jnp.zeros_like(grid)

    def operand(src, edges, group, y):
        up = (y + ny - 1) % ny
        down = (y + 1) % ny
        edge = left_edge[group]
        for pp in range(per_y):
            k = y * per_y + pp
            hpsi, own = [], []
            for t in range(2):
                p = 2 * pp + t
                r = y * cx + p
                here = src[r]
                before = edges[0, y] if p == 0 else src[r - 1]
                after = edges[1, y] if p == cx - 1 else src[r + 1]
                beside = before + after
                beside = beside + src[up * cx + p]
                beside = beside + src[down * cx + p]
                beside = beside + jnp.where(lanes % lane_half == 0, 0.0, pltpu.roll(here, 1, 1))
                beside = beside + pltpu.roll(here, nz - 1, 1)
                hpsi.append(0.5 * (6.0 * here - beside) + pot[p, pl.ds(y, 1)] * here)
                own.append(here)
                spot = (lanes == r) | (lanes == r + lane_half)
                edge = jnp.where(spot, -0.5 * pltpu.roll(here, (r + lane_half + 1) % nz, 1), edge)
            for slot, both in ((2 * group, pack(*hpsi)), (2 * group + 1, pack(*own))):
                for h in range(2):
                    high, low = parts(both[h])
                    lhs_high[h * half + k, pl.ds(slot * bands, bands)] = high
                    lhs_low[h * half + k, pl.ds(slot * bands, bands)] = low
        left_edge[group] = edge

    def accumulate(group, source, row, right_row, count):
        where = pl.ds(group * 2 * bands, 2 * bands)
        left, right = [], []
        for i in range(count):
            high, low = lhs_high[row + i, where], lhs_low[row + i, where]
            other_high, other_low = right_row(i)
            left += [high, high, low]
            right += [other_high, other_low, other_high]
        grid[source, where] += lax.dot_general(
            jnp.concatenate(left, axis=1), jnp.concatenate(right, axis=1), CONTRACT_LAST,
            preferred_element_type=jnp.float32,
        )

    def with_own(group, y, ys):
        own = pl.ds(bands, bands)
        for h in range(2):
            row = h * half + y * per_y
            accumulate(
                group, line, row, lambda i, row=row: (lhs_high[row + i, own], lhs_low[row + i, own]), ys * per_y
            )

    def with_moved(group, way, f, y, ys):
        accumulate(
            group, way.source(f), way.half_of(f) * half + y * per_y,
            lambda i: parts(way.slots[f, y * per_y + i]), ys * per_y,
        )

    def moved_all(group, f, y, ys):
        for way in ways:
            @pl.when(way.gets(f))
            def _(way=way):
                with_moved(group, way, f, y, ys)

    def partner_operand(y):
        both_planes(partner_halo, fwd_send, fwd_recv, y).wait_recv()
        operand(partner, partner_halo, 1, y)

    def with_edges(group):
        into = pl.ds(2 * group * bands, bands)
        low = low_lanes[: bands // 2]
        right = [full_edge[...]]
        found = []
        for way in ways:
            for f in range(phases):
                here = way.edges[f]
                turned = pltpu.roll(here, lane_half, 1)
                first = way.half_of(f) == 0
                keep = (low ^ (way.half_of(f) == 1)) & way.gets(f)
                right.append(jnp.where(keep, jnp.where(first, here, turned), 0.0))
                right.append(jnp.where(keep, jnp.where(first, turned, here), 0.0))
                found.append((way, f))
        added = three(parts(left_edge[group]), parts(jnp.concatenate(right, axis=0)), CONTRACT_LAST, 1)
        grid[line, into] += added[:, :bands]
        for at, (way, f) in enumerate(found):
            @pl.when(way.gets(f))
            def _(way=way, f=f, at=at):
                grid[way.source(f), into] += added[:, (at + 1) * bands : (at + 2) * bands]

    def edge_stage(f):
        for way in ways:
            @pl.when(way.gets(f))
            def _(way=way):
                way.edge_arrival(f).wait_recv()

            @pl.when(way.passes(f))
            def _(way=way):
                way.edge_hop(f).start()

    def couple(group):
        for kind in range(2):
            coupled = jnp.transpose(exact(sym[kind], coef[group]))
            high, low = parts(coupled)
            where = pl.ds((2 * group + kind) * bands, bands)
            coup_high[where] = high
            coup_low[where] = low

    def project(source, right):
        grid[source] += three((coup_high[...], coup_low[...]), parts(right), MATMUL, 0)

    def coef_stage(dist):
        @pl.when(line >= dist)
        def _():
            coef_hop(dist).wait_recv()

        if dist < hops:
            @pl.when((line >= dist) & (line < last))
            def _():
                coef_hop(dist + 1).start()

        @pl.when(line >= dist)
        def _():
            project(line - dist, coef_below[dist - 1])

    def partner_row(u, carry):
        swap(u).wait_recv()
        for copy in forwards(u):
            copy.start()

        @pl.when(u + swap_window < ny)
        def _():
            swap(u).wait_send()
            swap(u + swap_window).start()

        @pl.when(u >= 2)
        def _():
            partner_operand(u - 1)
            with_own(1, u - 1, 1)
            moved_all(1, 0, u - 1, 1)

        return carry

    def first_phase(t, carry):
        for y in (halo_ahead + 2 * t, halo_ahead + 2 * t + 1):
            @pl.when(y < ny)
            def _(y=y):
                for copy in halos(y):
                    copy.start()

        @pl.when(t >= 2)
        def _():
            take(0, 2 * t)

        for y in (2 * t, 2 * t + 1):
            both_planes(halo, halo_send, halo_recv, y).wait_recv()
            operand(nat, halo, 0, y)
        with_own(0, 2 * t, 2)

        @pl.when(t >= 2)
        def _():
            take(0, 2 * t + 1)

        @pl.when(t == 0)
        def _():
            take(0, 3)

        moved_all(0, 0, 2 * t, 2)
        partner_row(t, 0)
        return carry

    lax.fori_loop(0, steps, first_phase, 0)

    coef_swap.wait_recv()
    couple(0)
    couple(1)
    project(line, coef[0])
    edge_stage(0)
    coef_stage(1)

    def second_phase(t, carry):
        take(1, 2 * t)
        partner_row(steps + t, 0)
        take(1, 2 * t + 1)
        moved_all(0, 1, 2 * t, 2)
        for y in (2 * t, 2 * t + 1):
            @pl.when(y != 0)
            def _(y=y):
                moved_all(1, 1, y, 1)

        for stage in range(1, hops):
            @pl.when(t == min(2 * stage + 1, steps - 3))
            def _(stage=stage):
                if stage < phases:
                    edge_stage(stage)
                coef_stage(stage + 1)

        @pl.when(t == steps - 3)
        def _():
            with_edges(0)
            if fused:
                combine.first_send()

        return carry

    lax.fori_loop(0, steps - 1, second_phase, 0)
    between = (line > 0) & (line < last)
    take(1, ny - 2)
    if fused:
        combine.first_fold()
    partner_row(ny - 1, 0)

    @pl.when(between)
    def _():
        take(1, ny - 1)

    partner_operand(0)
    with_own(1, 0, 1)
    moved_all(1, 0, 0, 1)
    moved_all(1, 1, 0, 1)

    @pl.when(~between)
    def _():
        take(1, ny - 1)

    moved_all(0, 1, ny - 2, 2)
    early = fused and phases == 2
    if early:
        combine.send(0)
    partner_operand(ny - 1)
    with_own(1, ny - 1, 1)
    moved_all(1, 0, ny - 1, 1)
    if early:
        combine.reduce(0)
    moved_all(1, 1, ny - 2, 2)
    with_edges(1)
    for f in range(2, phases):
        def later_phase(t, carry, f=f):
            take(f, 2 * t)
            take(f, 2 * t + 1)
            moved_all(0, f, 2 * t, 2)
            moved_all(1, f, 2 * t, 2)
            return carry

        lax.fori_loop(0, steps, later_phase, 0)

    if fused:
        if not early:
            combine.send(0)
            combine.reduce(0)
        combine.send(1)
        combine.first_close()
        combine.reduce(1)
        combine.rest()

    for y in range(ny - swap_window, ny):
        swap(y).wait_send()
    remote(halo, halo, halo_send.at[0], halo_recv.at[0], {"dom": dom_next}).wait_send()
    remote(partner_halo, partner_halo, fwd_send.at[0], fwd_recv.at[0], {"dom": dom_next}).wait_send()
    for way in ways:
        @pl.when(way.own_first)
        def _(way=way):
            for ahead in range(window):
                way.sent(way.items - window + ahead)

        @pl.when(way.place == last - 1)
        def _(way=way):
            remote(
                way.slots, way.slots, way.send.at[window], way.recv.at[0, 0], {"band": way.to}
            ).wait_send()

    coef_swap.wait_send()
    for dist in range(1, lines):
        @pl.when((line >= dist - 1) & (line < last))
        def _(dist=dist):
            coef_hop(dist).wait_send()
    for way in ways:
        @pl.when(way.own_first)
        def _(way=way):
            way.own_edge().wait_send()

        @pl.when(way.place == 0)
        def _(way=way):
            way.extra_edge().wait_send()

        for f in range(phases):
            @pl.when(way.passes(f))
            def _(way=way, f=f):
                way.edge_hop(f).wait_send()


class Combine:
    def __init__(self, lines, volume, grid, out, line, side, pair, dom, scratch):
        (
            from_core, both, from_chip, total, mirror, swapped,
            core_send, core_recv, chip_send, chip_recv, line_send, line_recv, side_send, side_recv,
            near_send, near_recv, far_send, far_recv, pass_send, pass_recv, result, out_sem,
        ) = scratch
        bands = grid.shape[2]
        core = dom % 2
        kind = dom // 2
        other_core = kind * 2 + (1 - core)
        other_chip = (1 - kind) * 2 + core
        my_kind = pl.ds(pl.multiple_of(kind * bands, bands), bands)
        their_kind = pl.ds(pl.multiple_of((1 - kind) * bands, bands), bands)
        turn = jnp.where(line == 0, 1, 0)
        others = [(line + 1 + (k + turn) % (lines - 1)) % lines for k in range(lines - 1)]
        order = others + [line]
        closing = [line] + others

        def rows(group):
            return pl.ds(group * 2 * bands, 2 * bands)

        def to_core(group, s):
            return remote(
                grid.at[s, rows(group)], from_core.at[s], core_send.at[0], core_recv.at[s], {"dom": other_core}
            )

        def to_chip(s):
            return remote(both.at[s, their_kind], from_chip.at[s], chip_send.at[0], chip_recv.at[s], {"dom": other_chip})

        def to_line(s):
            return remote(
                total.at[s], mirror.at[line], line_send.at[0], line_recv.at[line], {"band": s * 2 + side}
            )

        def from_line(s):
            return remote(
                total.at[s], mirror.at[s], line_send.at[0], line_recv.at[s], {"band": s * 2 + side}
            )

        def to_side(s):
            return remote(total.at[s], swapped.at[s], side_send.at[0], side_recv.at[s], {"band": pair})

        def piece(s, group, k, send, recv, to):
            block = s * 2 + (side if group == 0 else 1 - side)
            at = result.at[k, :, pl.ds(pl.multiple_of(block * bands, bands), bands)]
            return remote(at, at, send.at[0], recv.at[s], {"dom": to})

        def near(s, group):
            return piece(s, group, kind, near_send, near_recv, other_core)

        def far(s, group, k):
            return piece(s, group, k, far_send, far_recv, other_chip)

        def onward(s, group):
            return piece(s, group, 1 - kind, pass_send, pass_recv, other_core)

        def blocks(group):
            return closing if group else others

        def send(group):
            @pl.when(core == 1 - group)
            def _():
                for s in order if group else others:
                    to_core(group, s).start()

        def flush(s, group, k):
            block = s * 2 + (side if group == 0 else 1 - side)
            at = (k, slice(None), pl.ds(pl.multiple_of(block * bands, bands), bands))
            pltpu.make_async_copy(result.at[at], out.at[at], out_sem.at[0]).start()

        def fold(group, s):
            to_core(group, s).wait_recv()
            both[s] = grid[s, rows(group)] + from_core[s]
            to_chip(s).start()

        def close(group, s, value):
            block = s * 2 + (side if group == 0 else 1 - side)
            result[kind, :, pl.ds(pl.multiple_of(block * bands, bands), bands)] = volume * value
            far(s, group, kind).start()
            near(s, group).start()
            flush(s, group, kind)

        def first_send():
            @pl.when(core == 1)
            def _():
                to_core(0, line).start()

        def first_fold():
            @pl.when(core == 0)
            def _():
                fold(0, line)

        def first_close():
            @pl.when(core == 0)
            def _():
                to_chip(line).wait_recv()
                close(0, line, both[line, my_kind] + from_chip[line])

        def reduce(group):
            @pl.when(core == group)
            def _():
                for s in order if group else others:
                    fold(group, s)

        def work(group):
            for s in order if group else others:
                to_chip(s).wait_recv()
                total[s] = both[s, my_kind] + from_chip[s]
                if s is not line:
                    to_line(s).start()
                if group:
                    to_side(s).start()
            for s in blocks(group):
                if group:
                    to_side(s).wait_recv()
                    value = swapped[s]
                else:
                    value = total[s]
                if s is not line:
                    from_line(s).wait_recv()
                    value = value + jnp.transpose(mirror[s])
                close(group, s, value)
            for s in closing:
                near(s, 1 - group).wait_recv()
                flush(s, 1 - group, kind)
            for s in closing:
                far(s, group, 1 - kind).wait_recv()
                onward(s, group).start()
                flush(s, group, 1 - kind)
            for s in closing:
                onward(s, 1 - group).wait_recv()
                flush(s, 1 - group, 1 - kind)
            pltpu.make_async_copy(result, result, out_sem.at[0]).wait()
            for held, send, recv in (
                (from_core, core_send, core_recv), (from_chip, chip_send, chip_recv),
                (mirror.at[pl.ds(0, lines - 1)], line_send, line_recv), (total, near_send, near_recv),
                (total, far_send, far_recv), (total, pass_send, pass_recv),
            ):
                remote(held, held, send.at[0], recv.at[0], {"dom": other_core}).wait_send()
            if group:
                remote(swapped, swapped, side_send.at[0], side_recv.at[0], {"dom": other_core}).wait_send()

        def rest():
            for group in range(2):
                @pl.when(core == group)
                def _(group=group):
                    work(group)

        self.send = send
        self.first_send, self.first_fold, self.first_close = first_send, first_fold, first_close
        self.reduce = reduce
        self.rest = rest


def gram(psi, pot, proj, ham_corr, delta, counts, lines, doms, fused, volume):
    bands, cx, ny, nz = psi.shape
    rows = cx * ny
    half = rows // 2
    used = proj.shape[0]
    width = -(-used // 128) * 128
    hops = lines - 1
    phases = lines - 2
    window = min(WINDOW, ny) + 1
    f32 = jnp.float32
    dma = pltpu.SemaphoreType.DMA
    vmem = pl.BlockSpec(memory_space=pltpu.VMEM)
    hbm = pl.BlockSpec(memory_space=pl.ANY)
    scratch = [
        pltpu.VMEM((rows, bands, nz), f32),
        pltpu.VMEM((2, half, bands, nz), f32),
        pltpu.VMEM((rows, bands, nz), f32),
        pltpu.VMEM((2, ny, bands, nz), f32),
        pltpu.VMEM((2, ny, bands, nz), f32),
        pltpu.VMEM((phases, half, bands, nz), f32),
        pltpu.VMEM((phases, half, bands, nz), f32),
        pltpu.VMEM((rows, QUADS * bands, nz), jnp.bfloat16),
        pltpu.VMEM((rows, QUADS * bands, nz), jnp.bfloat16),
        pltpu.VMEM((2, bands // 2, nz), f32),
        pltpu.VMEM((bands, nz), f32),
        pltpu.VMEM((2, bands, nz), f32),
        pltpu.VMEM((phases, bands // 2, nz), f32),
        pltpu.VMEM((phases, bands // 2, nz), f32),
        pltpu.VMEM((rows, used, nz), f32),
        pltpu.VMEM((2, width, width), f32),
        pltpu.VMEM((2, width, bands), f32),
        pltpu.VMEM((hops, width, bands), f32),
        pltpu.VMEM((QUADS * bands, width), jnp.bfloat16),
        pltpu.VMEM((QUADS * bands, width), jnp.bfloat16),
        dma((ny,)), dma((1,)), dma((min(SWAP_WINDOW, ny),)), dma((ny,)), dma((1,)), dma((ny,)), dma((1,)), dma((ny,)),
        dma((window,)), dma((phases, ny)), dma((window,)), dma((phases, ny)),
        dma((phases,)), dma((phases,)), dma((phases,)), dma((phases,)),
        dma((hops,)), dma((hops,)), dma((1,)), dma((1,)),
    ]
    if fused:
        columns = 2 * lines * bands
        shape = jax.ShapeDtypeStruct((2, bands, columns), f32)
        placed = hbm
        scratch += [
            pltpu.VMEM((lines, QUADS * bands, bands), f32),
            pltpu.VMEM((lines, 2 * bands, bands), f32),
            pltpu.VMEM((lines, 2 * bands, bands), f32),
            pltpu.VMEM((lines, bands, bands), f32),
            pltpu.VMEM((lines, bands, bands), f32),
            pltpu.VMEM((lines, bands, bands), f32),
            pltpu.VMEM((lines, bands, bands), f32),
        ] + [dma((1,)), dma((lines,))] * 7 + [pltpu.VMEM((2, bands, columns), f32), dma((1,))]
    else:
        shape = jax.ShapeDtypeStruct((lines, QUADS * bands, bands), f32)
        placed = vmem
    return pl.pallas_call(
        functools.partial(gram_kernel, lines, doms, fused, volume),
        out_shape=shape,
        in_specs=[pl.BlockSpec(memory_space=pltpu.SMEM), hbm, vmem, hbm, vmem, vmem],
        out_specs=placed,
        scratch_shapes=scratch,
        compiler_params=pltpu.CompilerParams(
            collective_id=0, has_side_effects=True, vmem_limit_bytes=62 * 1024 * 1024
        ),
    )(counts, psi, pot, proj, ham_corr, delta)


def on_device(
    wavefunctions, potential, projectors, hamiltonian_correction, delta_s, projector_count
):
    bands, cx, ny, nz = wavefunctions.shape
    groups = lax.axis_size("band")
    doms = lax.axis_size("dom")
    lines = groups // 2
    mine = lax.axis_index("band")
    line, side = mine // 2, mine % 2
    volume = 1.0 / (cx * ny * nz * doms)
    atoms, slots = hamiltonian_correction.shape[:2]
    proj = projectors.reshape(atoms * slots, cx, ny, nz)
    fused = doms == QUADS and bands % 128 == 0
    grid = gram(
        wavefunctions, potential, proj, jnp.transpose(hamiltonian_correction, (1, 0, 2)),
        jnp.transpose(delta_s, (1, 0, 2)), projector_count, lines, doms, fused, volume,
    )
    if fused:
        return grid[0], grid[1]
    here = (jnp.arange(lines, dtype=jnp.int32) == line)[:, None, None, None]
    both = lax.psum(grid.reshape(lines, QUADS, bands, bands), "dom")
    lanes = [[at * 2 + s for at in range(lines)] for s in range(2)]
    mirrored = lax.all_to_all(both, "band", 0, 0, axis_index_groups=lanes, tiled=True)
    swapped = lax.ppermute(both, "band", [(i, i ^ 1) for i in range(groups)])
    crossed = (jnp.arange(QUADS, dtype=jnp.int32) >= 2)[None, :, None, None]
    total = volume * jnp.where(crossed, swapped, both) + volume * jnp.where(here, 0.0, jnp.swapaxes(mirrored, 2, 3))
    total = total.reshape(lines, 2, 2, bands, bands)
    by_side = jnp.where(side == 0, total, total[:, ::-1])
    final = jnp.transpose(by_side, (2, 3, 0, 1, 4)).reshape(2, bands, groups * bands)
    return final[0], final[1]


def solution(mesh):
    placed = (
        P("band", "dom", None, None),
        P("dom", None, None),
        P("dom", None, None, None, None),
        P("dom", None, None),
        P("dom", None, None),
        P("dom"),
    )
    return jax.shard_map(
        on_device,
        mesh=mesh,
        in_specs=placed,
        out_specs=(P("band", None), P("band", None)),
        check_vma=False,
    )
```
